512 devices in a mesh: row: 32 (over z, y_lo, core), col: 16 (over x, y_hi).
Axes of the slice: x: 4, y: 8 (y_hi: 4, y_lo: 2; y = y_hi * 2 + y_lo), z: 8, core: 2. Of those that a mesh axis runs over, the one named last changes fastest.
Arguments:
- pair_exchange: bfloat16 [1024, 16, 1024], P(('row', 'col')), may hold values from -6 to 6
- conduction: bfloat16 [1024, 4, 1024], P(('row', 'col')), may hold values from -6 to 6
- valence: bfloat16 [1024, 4, 1024], P(('row', 'col')), may hold values from -6 to 6
- coulomb: float32 [1024], replicated, may hold values from 0.5 to 5
- screening: float32 [289, 1024], replicated, may hold values from 0.1 to 1
- energies: float32 [1024, 16], P(('row', 'col')), may hold values from 1 to 9
- vectors: bfloat16 [1024, 512], P(('row', 'col')), may hold values from -6 to 6
- k_coords: int32 [1024, 2], P(('row', 'col')), may hold values from 0 to 31, as said below
Outputs:
- residual_block: float32 [1024, 512], P(('row', 'col'))
- alpha: float32 [32, 32], replicated
The draws below stay inside these ranges and needn't reach their ends.
Inputs may be any that keep to these rules, and one draw needn't show every extreme that they name: `k_coords`: each row holds a k-point's coordinates on the periodic 32 x 32 mesh, first then second; every mesh point occurs exactly once.
All inputs are finite; a program needn't handle non-finite values.
Results may differ from the reference program's by a relative error of at most 0.0028.
Values may be sent and summed in bfloat16 or wider, within the bound.
A program may use at most 64 MiB of HBM per device.

```python
import math
import jax
import jax.numpy as jnp
from jax import lax

NV = 4
NC = 4
NB = 16
NG = 1024
NVEC = 32
MX = 32
NK = 1024
MY = 32
NT = 16384
NQF = 289


def draw_energies(key, part):
    ramp = 1.0 + 2.0 * jnp.arange(NK, dtype=jnp.float32)[:, None] / NK
    base = jnp.exp(jax.random.uniform(key, (NK, NB), jnp.float32, 0.0, math.log(3.0)))
    return (base * ramp).astype(jnp.float32)


def draw_k_coords(key, part):
    order = jax.random.permutation(key, NK)
    return jnp.stack([order // MY, order % MY], axis=1).astype(jnp.int32)


def block_levels(key, dims, shards, least, largest):
    level = 1.0
    for axis_at, blocks in shards:
        draws = jax.random.uniform(jax.random.fold_in(jax.random.fold_in(key, 6), axis_at), (blocks,), jnp.float32, least / len(shards), largest / len(shards))
        level = level * jnp.repeat(jnp.exp(draws), dims[axis_at] // blocks).reshape((-1,) + (1,) * (len(dims) - 1 - axis_at))
    return level


def bell_draw(own_key, extent, spread, limit, cuts=(), kind=jnp.bfloat16):
    factor_of = block_levels(own_key, extent, cuts, -0.22, 0.18) if cuts else 1.0
    values = jax.random.normal(own_key, extent, jnp.float32) * spread * factor_of
    return jnp.minimum(jnp.maximum(values, -limit), limit).astype(kind)


def setup_inputs(seed: int = 0) -> dict:
    key_of = jax.random.split(jax.random.key(seed), 9)
    pair_exchange = bell_draw(key_of[0], (NK, NB, NG), 1.0, 6.0, ((0, 512),))
    conduction = bell_draw(key_of[1], (NK, NC, NG), 1.0, 6.0, ((0, 512),))
    valence = bell_draw(key_of[2], (NK, NV, NG), 1.0, 6.0, ((0, 512),))
    coulomb = jnp.clip(jnp.exp(jax.random.uniform(key_of[3], (NG,), jnp.float32, math.log(0.5), math.log(5.0))), 0.5, 5.0)
    screening = jnp.clip(jnp.exp(jax.random.uniform(key_of[4], (NQF, NG), jnp.float32, math.log(0.1), math.log(1.0))), 0.1, 1.0)
    energies = draw_energies(jax.random.fold_in(key_of[8], 71), 0)
    vectors = bell_draw(key_of[6], (NK, NB * NVEC), 1.0, 6.0, ((0, 512),))
    k_coords = draw_k_coords(jax.random.fold_in(key_of[8], 71), 0)
    return dict(pair_exchange=pair_exchange, conduction=conduction, valence=valence, coulomb=coulomb, screening=screening, energies=energies, vectors=vectors, k_coords=k_coords)


highest = lax.Precision.HIGHEST


def reference(pair_exchange, conduction, valence, coulomb, screening, energies, vectors, k_coords):
    moving = vectors.astype(jnp.float32).reshape(NK, NB, NVEC)
    joined = (valence.astype(jnp.float32)[:, :, None, :] * conduction.astype(jnp.float32)[:, None, :, :]).reshape(NK, NB, NG)
    pair_rows = lax.optimization_barrier(joined.astype(jnp.bfloat16)).astype(jnp.float32)
    along_first = jnp.arange(MX)
    along_second = jnp.arange(MY)
    fold_first = jnp.minimum(along_first, MX - along_first)
    fold_second = jnp.minimum(along_second, MY - along_second)
    mesh_index = (fold_first[:, None] * (MY // 2 + 1) + fold_second[None, :]).astype(jnp.int32)
    spectrum = jnp.fft.fft2(screening[mesh_index], axes=(0, 1)).real
    density = jnp.einsum("ktg,ktn->gn", pair_exchange.astype(jnp.float32), moving, precision=highest)
    place_first = k_coords[:, 0]
    place_second = k_coords[:, 1]
    block_size = 64 if NG % 64 == 0 else NG

    def one_block(running, anchor):
        piece_rows = lax.dynamic_slice_in_dim(pair_rows, anchor, block_size, 2)
        projected = jnp.einsum("ktg,ktn->kgn", piece_rows, moving, precision=highest)
        mesh_grid = jnp.zeros((MX, MY, block_size, NVEC), jnp.float32).at[place_first, place_second].set(projected)
        spectrum_part = lax.dynamic_slice_in_dim(spectrum, anchor, block_size, 2)
        potential = jnp.fft.ifft2(jnp.fft.fft2(mesh_grid, axes=(0, 1)) * spectrum_part[:, :, :, None], axes=(0, 1)).real
        sampled = potential[place_first, place_second]
        return running + jnp.einsum("ktg,kgn->ktn", piece_rows, sampled, precision=highest), None

    anchors = (jnp.arange(NG // block_size) * block_size).astype(jnp.int32)
    direct, _ = lax.scan(one_block, jnp.zeros((NK, NB, NVEC), jnp.float32), anchors)
    exchange_term = jnp.einsum("ktg,gn->ktn", pair_exchange.astype(jnp.float32) * coulomb, density, precision=highest)
    applied = energies[:, :, None] * moving + (2.0 / NT) * exchange_term - direct / NK
    alpha = jnp.einsum("ktm,ktn->mn", moving, applied, precision=highest) / NT
    residual = applied - jnp.einsum("ktm,mn->ktn", moving, alpha, precision=highest)
    return residual.reshape(NK, NB * NVEC), alpha
```

```python
import jax
import jax.numpy as jnp
import numpy as np
from jax import lax
from jax.experimental import pallas as pl
from jax.experimental.pallas import tpu as pltpu
from jax.sharding import PartitionSpec as P

MESH = pl.DeviceIdType.MESH
HIGH = lax.Precision.HIGHEST
F32 = jnp.float32
BF16 = jnp.bfloat16

NR, NC = 32, 16
NK, NT = 1024, 16384
NQ = 289
QPAD = 384
X_COORD_ROW, X_COORD_COL, X_PROJ_ROW, X_PROJ_COL, X_DENS_ROW, X_DENS_COL, X_DENS_OUT = range(7)
X_POT_COL, X_POT_ROW, X_ALPHA_COL, X_ALPHA_ROW = range(7, 11)


def real_basis():
    points = np.arange(32)[None, :]
    order = np.arange(32)[:, None]
    freq = np.where(order <= 16, order, order - 16)
    angle = 2 * np.pi * freq * points / 32
    basis = np.where(order <= 16, np.cos(angle), np.sin(angle)) * np.sqrt(2 / 32)
    basis[[0, 16]] *= np.sqrt(0.5)
    return basis, freq[:, 0]


def two_parts(table):
    high = table.astype(BF16)
    return high, (table - high.astype(np.float64)).astype(BF16)


def tables():
    basis, freq = real_basis()
    fold = np.arange(17)
    weight = np.where((fold == 0) | (fold == 16), 1.0, 2.0)
    cosine = weight[None, :] * np.cos(2 * np.pi * freq[:, None] * fold[None, :] / 32)
    modes = np.zeros((NK, QPAD))
    modes[:, :NQ] = np.kron(cosine, cosine)
    return np.concatenate(two_parts(basis), axis=1), *two_parts(modes)


def iota(shape, dim):
    return lax.broadcasted_iota(jnp.int32, shape, dim)


def one_hot(mask):
    return jnp.where(mask, 1.0, 0.0).astype(F32)


def dot(a, b, ca=1, cb=0, precision=None):
    return lax.dot_general(
        a, b, (((ca,), (cb,)), ((), ())), precision=precision, preferred_element_type=F32
    )


def split(v):
    high = v.astype(BF16)
    return high, (v - high.astype(F32)).astype(BF16)


def fold(v, *shifts):
    for shift in shifts:
        v = v + pltpu.roll(v, shift, 1)
    return v


def kernel(
    pe_ref, cond_ref, val_ref, coul_ref, en_ref, vec_ref, kc_ref, q2_ref, scr_hbm, mhi_hbm, mlo_hbm,
    out_ref, alpha_ref,
    v8, pairs, lk, pk, coulexp, c8,
    p_out, p_in, q_out, q_in, d_out, d_in, e_out, e_in, f_out, f_in,
    k_out, k_in, h_out, h_in, c16,
    z_out, z_in, y_out, y_in, a_out, a_in, b_out, b_in,
    arow, brow, tt_hi, tt_lo, lam, wt, perm_f, perm_b, scr, m_hi, m_lo,
    send_sems, recv_sems, local_sems,
):
    r, c = lax.axis_index("row"), lax.axis_index("col")
    sizes = {"row": (NR, r), "col": (NC, c)}

    def peers(axis, body):
        size, me = sizes[axis]
        half = size // 2

        def step(i, carry):
            ahead = jnp.where(i < half, half + i, i - half + 1)
            body(lax.rem(me + ahead, size))
            return carry

        lax.fori_loop(0, size - 1, step, 0)

    def send(axis, which, source, target):
        me = sizes[axis][1]

        def one(peer):
            pltpu.make_async_remote_copy(
                src_ref=source(peer),
                dst_ref=target.at[me],
                send_sem=send_sems.at[which],
                recv_sem=recv_sems.at[which],
                device_id={axis: peer},
                device_id_type=MESH,
            ).start()

        peers(axis, one)

    def wait_all(axis, sems, which, target):
        many = target.at[pl.ds(0, sizes[axis][0] - 1)]
        pltpu.make_async_copy(many, many, sems.at[which]).wait()

    def arrived(axis, which, target):
        wait_all(axis, recv_sems, which, target)

    barrier = pltpu.get_barrier_semaphore()
    for axis in ("row", "col"):
        peers(
            axis,
            lambda peer, axis=axis: pl.semaphore_signal(
                barrier, inc=1, device_id={axis: peer}, device_id_type=MESH
            ),
        )
    near = pl.multiple_of((r // 8) * 128, 128)
    far = pl.multiple_of((r // 8) * 128 + 512, 128)
    fetches = [
        pltpu.make_async_copy(
            scr_hbm.at[:, pl.ds(near, 128)], scr.at[0, pl.ds(0, NQ), :], local_sems.at[0]
        ),
        pltpu.make_async_copy(
            scr_hbm.at[:, pl.ds(far, 128)], scr.at[1, pl.ds(0, NQ), :], local_sems.at[1]
        ),
        pltpu.make_async_copy(mhi_hbm, m_hi, local_sems.at[2]),
        pltpu.make_async_copy(mlo_hbm, m_lo, local_sems.at[3]),
    ]
    for fetch in fetches:
        fetch.start()

    place = iota((1, 128), 1) - 4 * r
    k_row = jnp.zeros((1, 128), jnp.int32)
    for q in range(4):
        k_row = jnp.where(place == q, kc_ref[q // 2, q % 2], k_row)
    k_out[...] = k_row.astype(F32)

    vec = vec_ref[...].astype(F32)
    for i in range(8):
        v8[i : i + 1, :] = vec[i // 4 : i // 4 + 1, (i % 4) * 128 : (i % 4 + 1) * 128]
    row32, lane32 = iota((32, 128), 0), iota((32, 128), 1)
    lane_is_t = (row32 & 3) == (lane32 >> 5)
    spread = one_hot((iota((32, 8), 0) >> 2) == iota((32, 8), 1))
    gather8 = one_hot((iota((8, 32), 1) >> 2) == iota((8, 32), 0))
    wide = dot(spread.astype(BF16), v8[...].astype(BF16))
    x128 = fold(jnp.where(lane_is_t, wide, 0.0), 64, 32)

    for k in range(2):
        cond = cond_ref[k].astype(F32)
        val = val_ref[k].astype(F32)
        for v in range(4):
            at = 16 * k + 4 * v
            pairs[at : at + 4, :] = val[v : v + 1, :] * cond
    pair_rows = pairs[...].astype(BF16)
    lk[0:32, :] = pair_rows[:, :512]
    lk[32:64, :] = pair_rows[:, 512:]
    row64, lane64 = iota((64, 128), 0), iota((64, 128), 1)
    own64 = ((row64 >> 5) == ((lane64 >> 5) & 1)) & (((row64 >> 4) & 1) == (lane64 >> 6))
    x_block = jnp.where(own64, jnp.concatenate([x128, x128], axis=0), 0.0).astype(BF16)
    p_out[...] = dot(lk[...], x_block, 0, 0).astype(BF16).reshape(NR, NC, 128)

    for k in range(2):
        for j in range(4):
            at = 32 * j + 16 * k
            pk[at : at + 16, :] = pe_ref[k, :, j * 256 : (j + 1) * 256]
    own128 = (iota((128, 128), 0) >> 5) == (iota((128, 128), 1) >> 5)
    x_quarter = jnp.where(own128, jnp.concatenate([x128] * 4, axis=0), 0.0).astype(BF16)
    d_out[...] = dot(pk[...], x_quarter, 0, 0).reshape(NR, 8, 128)

    pl.semaphore_wait(barrier, NR + NC - 2)
    send("row", X_COORD_ROW, lambda peer: k_out, k_in)
    send("row", X_PROJ_ROW, lambda peer: p_out.at[peer], p_in)
    send("row", X_DENS_ROW, lambda peer: d_out.at[peer], d_in)
    k_in[pl.ds(r, 1)] = k_out[...].reshape(1, 1, 128)
    p_in[pl.ds(r, 1)] = p_out[pl.ds(r, 1)]
    d_in[pl.ds(r, 1)] = d_out[pl.ds(r, 1)]

    def build_perm(i, carry):
        at = pl.multiple_of(i * 128, 128)
        row, col = iota((128, 512), 0) + i * 128, iota((128, 512), 1)
        perm_f[pl.ds(at, 128), :] = one_hot(col == ((row & 31) << 4) + (row >> 5)).astype(BF16)
        perm_b[pl.ds(at, 128), :] = one_hot(col == ((row & 15) << 5) + (row >> 4)).astype(BF16)
        return carry

    lax.fori_loop(0, 4, build_perm, 0)
    c8[...] = jnp.zeros((8, 256), F32)
    for j in range(4):
        c8[j : j + 1, :] = coul_ref[:, j * 256 : (j + 1) * 256]
    expand8 = one_hot(iota((8, 128), 0) == (iota((8, 128), 1) >> 5))
    coulexp[...] = dot(c8[...], expand8, 0, 0, precision=HIGH)

    energy = jnp.concatenate(
        [jnp.broadcast_to(en_ref[k : k + 1, :], (16, 16)) for k in range(2)], axis=0
    )
    same = (iota((32, 16), 0) & 15) == iota((32, 16), 1)
    e_col = jnp.sum(jnp.where(same, energy, 0.0), axis=1, keepdims=True)
    ex128 = e_col * x128
    alpha_energy = dot(x128, ex128, 0, 0, precision=HIGH)[:32]

    arrived("row", X_COORD_ROW, k_in)
    h_out[...] = jnp.sum(k_in[...], axis=0)
    send("col", X_COORD_COL, lambda peer: h_out, h_in)
    h_in[pl.ds(c, 1)] = h_out[...].reshape(1, 1, 128)

    for fetch in fetches:
        fetch.wait()
    chosen = (r % 8) * 16 + c
    seen = (iota((QPAD, 128), 0) < NQ) & (iota((QPAD, 128), 1) == chosen)
    columns = [jnp.sum(jnp.where(seen, scr[h], 0.0), axis=1, keepdims=True) for h in range(2)]
    lane_q = iota((QPAD, 128), 1)
    s_hi, s_lo = split(jnp.where(((lane_q >> 5) & 1) == 0, columns[0], columns[1]))

    def build_lam(i, carry):
        at = pl.multiple_of(i * 256, 256)
        high, low = m_hi[pl.ds(at, 256), :], m_lo[pl.ds(at, 256), :]
        lam[pl.ds(at, 256), :] = dot(high, s_hi) + dot(high, s_lo) + dot(low, s_hi)
        return carry

    lax.fori_loop(0, 4, build_lam, 0)

    arrived("row", X_PROJ_ROW, p_in)
    mixed = dot(perm_f[...], p_in[...].reshape(512, 128)).astype(BF16)
    q_out[...] = mixed.reshape(NC, NR, 128)
    send("col", X_PROJ_COL, lambda peer: q_out.at[peer], q_in)
    q_in[pl.ds(c, 1)] = q_out[pl.ds(c, 1)]
    arrived("row", X_DENS_ROW, d_in)
    e_out[...] = jnp.sum(d_in[...], axis=0)
    send("col", X_DENS_COL, lambda peer: e_out, e_in)
    e_in[pl.ds(c, 1)] = e_out[...].reshape(1, 8, 128)

    arrived("col", X_COORD_COL, h_in)
    for i in range(NC):
        c16[i : i + 1, :] = h_in[i]
    repeat = one_hot(iota((16, 512), 0) == (iota((16, 512), 1) >> 5)).astype(BF16)
    spread_c = dot(c16[...].astype(BF16), repeat, 0, 0)
    row128, lane512 = iota((128, 512), 0), iota((128, 512), 1)
    kept = jnp.where((row128 >> 2) == (lane512 & 31), spread_c, 0.0).astype(BF16)
    pick = one_hot((iota((128, 128), 0) >> 5) == (iota((128, 128), 1) & 3)).astype(BF16)
    coords = dot(pick, kept)
    hot = one_hot(coords == (row128 & 31).astype(F32)).astype(BF16)
    q2 = q2_ref[...]
    for k in range(2):
        at = 64 * k
        first, second = hot[at : at + 32], hot[at + 32 : at + 64]
        arow[k] = dot(q2, jnp.concatenate([first, first], axis=0))
        brow[k] = dot(q2, jnp.concatenate([second, second], axis=0))

    def build_basis(j, carry):
        at = pl.multiple_of(j * 32, 32)
        for k in range(2):
            high, low = split(arow[k, pl.ds(j, 1), :] * brow[k])
            tt_hi[k, pl.ds(at, 32), :] = high
            tt_lo[k, pl.ds(at, 32), :] = low
        return carry

    lax.fori_loop(0, 32, build_basis, 0)

    arrived("col", X_PROJ_COL, q_in)
    proj = q_in[...].reshape(512, 128)
    lane256 = iota((256, 128), 1)

    def one_block(i, total):
        at = pl.multiple_of(i * 256, 256)
        parts = [
            dot(tt_hi[k, pl.ds(at, 256), :], proj) + dot(tt_lo[k, pl.ds(at, 256), :], proj)
            for k in range(2)
        ]
        mode = fold(jnp.where(lane256 < 64, parts[0], parts[1]), 64)
        scaled = lam[pl.ds(at, 256), :] * mode
        high, low = split(jnp.transpose(scaled)[:64])
        wt[0:64, pl.ds(at, 256)] = high
        wt[64:128, pl.ds(at, 256)] = low
        return total + dot(mode.astype(BF16), scaled.astype(BF16), 0, 0)

    alpha_direct = lax.fori_loop(0, 4, one_block, jnp.zeros((128, 128), F32))
    for k in range(2):
        both = dot(wt[...], tt_hi[k])
        back = both[:64] + both[64:] + dot(wt[0:64, :], tt_lo[k])
        coords_free = jnp.transpose(back)
        brow_at = 64 * k
        lam[0:512, brow_at : brow_at + 64] = coords_free
    z_out[...] = lam[0:512, :].astype(BF16).reshape(NC, NR, 128)
    send("col", X_POT_COL, lambda peer: z_out.at[peer], z_in)
    z_in[pl.ds(c, 1)] = z_out[pl.ds(c, 1)]

    mine = jnp.where((row64 >> 5) == ((lane64 >> 5) & 1), alpha_direct[:64], 0.0)
    part = alpha_energy - fold(mine[:32] + mine[32:], 32) * (1.0 / NK)
    a_out[...] = dot(gather8, jnp.where(lane_is_t, part, 0.0), precision=HIGH)
    send("col", X_ALPHA_COL, lambda peer: a_out, a_in)
    a_in[pl.ds(c, 1)] = a_out[...].reshape(1, 8, 128)

    arrived("col", X_DENS_COL, e_in)
    f_out[...] = jnp.sum(e_in[...], axis=0)
    send("row", X_DENS_OUT, lambda peer: f_out, f_in)
    f_in[pl.ds(r, 1)] = f_out[...].reshape(1, 8, 128)

    arrived("col", X_POT_COL, z_in)
    mixed = dot(perm_b[...], z_in[...].reshape(512, 128)).astype(BF16)
    y_out[...] = mixed.reshape(NR, NC, 128)
    send("row", X_POT_ROW, lambda peer: y_out.at[peer], y_in)
    y_in[pl.ds(r, 1)] = y_out[pl.ds(r, 1)]
    arrived("col", X_ALPHA_COL, a_in)
    b_out[...] = jnp.sum(a_in[...], axis=0)
    send("row", X_ALPHA_ROW, lambda peer: b_out, b_in)
    b_in[pl.ds(r, 1)] = b_out[...].reshape(1, 8, 128)

    arrived("row", X_DENS_OUT, f_in)
    density = f_in[...].reshape(256, 128)
    weighted = coulexp[...] * density
    w_hi, w_lo = split(weighted)
    quarters = pk[...]

    def total_of(v):
        v = jnp.where(own128, v, 0.0)
        return fold(v[0:32] + v[32:64] + v[64:96] + v[96:128], 64, 32)

    exchange = total_of(dot(quarters, w_hi) + dot(quarters, w_lo))
    alpha_exchange = total_of(dot(density, weighted, 0, 0, precision=HIGH))

    arrived("row", X_ALPHA_ROW, b_in)
    shares = dot(spread, jnp.sum(b_in[...], axis=0), precision=HIGH)
    shares = fold(jnp.where(lane_is_t, shares, 0.0), 64, 32)
    alpha = (shares + (2.0 / NT) * alpha_exchange) * (1.0 / NT)
    alpha_ref[...] = alpha[:, :32]
    base = ex128 + (2.0 / NT) * exchange - dot(x128[:, :32], alpha, precision=HIGH)

    arrived("row", X_POT_ROW, y_in)
    direct = jnp.where(own64, dot(lk[...], y_in[...].reshape(512, 128)), 0.0)
    residual = base - fold(direct[:32] + direct[32:], 64, 32) * (1.0 / NK)
    rows = dot(gather8, jnp.where(lane_is_t, residual, 0.0), precision=HIGH)
    for i in range(8):
        out_ref[i // 4 : i // 4 + 1, (i % 4) * 128 : (i % 4 + 1) * 128] = rows[i : i + 1, :]

    for axis, which, target in (
        ("row", X_COORD_ROW, k_in),
        ("row", X_PROJ_ROW, p_in),
        ("row", X_DENS_ROW, d_in),
        ("col", X_COORD_COL, h_in),
        ("col", X_PROJ_COL, q_in),
        ("col", X_DENS_COL, e_in),
        ("row", X_DENS_OUT, f_in),
        ("col", X_POT_COL, z_in),
        ("row", X_POT_ROW, y_in),
        ("col", X_ALPHA_COL, a_in),
        ("row", X_ALPHA_ROW, b_in),
    ):
        wait_all(axis, send_sems, which, target)


def on_device(pair_exchange, conduction, valence, coulomb, screening, energies, vectors, k_coords):
    q2, m_hi, m_lo = tables()
    vmem = pl.BlockSpec(memory_space=pltpu.VMEM)
    smem = pl.BlockSpec(memory_space=pltpu.SMEM)
    anywhere = pl.BlockSpec(memory_space=pl.ANY)
    return pl.pallas_call(
        kernel,
        out_shape=(
            jax.ShapeDtypeStruct((2, 512), F32),
            jax.ShapeDtypeStruct((32, 32), F32),
        ),
        in_specs=[vmem] * 6 + [smem, vmem] + [anywhere] * 3,
        out_specs=(vmem, vmem),
        scratch_shapes=[
            pltpu.VMEM((8, 128), F32),
            pltpu.VMEM((32, 1024), F32),
            pltpu.VMEM((64, 512), BF16),
            pltpu.VMEM((128, 256), BF16),
            pltpu.VMEM((256, 128), F32),
            pltpu.VMEM((8, 256), F32),
            pltpu.VMEM((NR, NC, 128), BF16),
            pltpu.VMEM((NR, NC, 128), BF16),
            pltpu.VMEM((NC, NR, 128), BF16),
            pltpu.VMEM((NC, NR, 128), BF16),
            pltpu.VMEM((NR, 8, 128), F32),
            pltpu.VMEM((NR, 8, 128), F32),
            pltpu.VMEM((8, 128), F32),
            pltpu.VMEM((NC, 8, 128), F32),
            pltpu.VMEM((8, 128), F32),
            pltpu.VMEM((NR, 8, 128), F32),
            pltpu.VMEM((1, 128), F32),
            pltpu.VMEM((NR, 1, 128), F32),
            pltpu.VMEM((1, 128), F32),
            pltpu.VMEM((NC, 1, 128), F32),
            pltpu.VMEM((16, 128), F32),
            pltpu.VMEM((NC, NR, 128), BF16),
            pltpu.VMEM((NC, NR, 128), BF16),
            pltpu.VMEM((NR, NC, 128), BF16),
            pltpu.VMEM((NR, NC, 128), BF16),
            pltpu.VMEM((8, 128), F32),
            pltpu.VMEM((NC, 8, 128), F32),
            pltpu.VMEM((8, 128), F32),
            pltpu.VMEM((NR, 8, 128), F32),
            pltpu.VMEM((2, 32, 512), F32),
            pltpu.VMEM((2, 32, 512), F32),
            pltpu.VMEM((2, NK, 512), BF16),
            pltpu.VMEM((2, NK, 512), BF16),
            pltpu.VMEM((NK, 128), F32),
            pltpu.VMEM((128, NK), BF16),
            pltpu.VMEM((512, 512), BF16),
            pltpu.VMEM((512, 512), BF16),
            pltpu.VMEM((2, QPAD, 128), F32),
            pltpu.VMEM((NK, QPAD), BF16),
            pltpu.VMEM((NK, QPAD), BF16),
            pltpu.SemaphoreType.DMA((11,)),
            pltpu.SemaphoreType.DMA((11,)),
            pltpu.SemaphoreType.DMA((4,)),
        ],
        compiler_params=pltpu.CompilerParams(
            collective_id=0, has_side_effects=True, vmem_limit_bytes=56 * 1024 * 1024
        ),
    )(
        pair_exchange,
        conduction,
        valence,
        coulomb.reshape(1, -1),
        energies,
        vectors,
        k_coords,
        jnp.asarray(q2),
        screening,
        jnp.asarray(m_hi),
        jnp.asarray(m_lo),
    )


def solution(mesh):
    split_k = ("row", "col")
    return jax.shard_map(
        on_device,
        mesh=mesh,
        in_specs=(
            P(split_k, None, None),
            P(split_k, None, None),
            P(split_k, None, None),
            P(),
            P(),
            P(split_k, None),
            P(split_k, None),
            P(split_k, None),
        ),
        out_specs=(P(split_k, None), P()),
        check_vma=False,
    )
```

```python
import jax
import jax.numpy as jnp
import numpy as np
from jax import lax
from jax.experimental import pallas as pl
from jax.experimental.pallas import tpu as pltpu
from jax.sharding import PartitionSpec as P

MESH = pl.DeviceIdType.MESH
HIGH = lax.Precision.HIGHEST
F32 = jnp.float32
BF16 = jnp.bfloat16

NR, NC = 32, 16
NK, NT = 1024, 16384
NQ = 289
QPAD = 384
X_COORD_ROW, X_COORD_COL, X_PROJ_ROW, X_PROJ_COL, X_DENS_ROW, X_DENS_COL, X_DENS_OUT = range(7)
X_POT_COL, X_POT_ROW, X_ALPHA_ROW, X_ALPHA_COL = range(7, 11)


def real_basis():
    points = np.arange(32)[None, :]
    order = np.arange(32)[:, None]
    freq = np.where(order <= 16, order, order - 16)
    angle = 2 * np.pi * freq * points / 32
    basis = np.where(order <= 16, np.cos(angle), np.sin(angle)) * np.sqrt(2 / 32)
    basis[[0, 16]] *= np.sqrt(0.5)
    return basis, freq[:, 0]


def two_parts(table):
    high = table.astype(BF16)
    return high, (table - high.astype(np.float64)).astype(BF16)


def tables():
    basis, freq = real_basis()
    fold = np.arange(17)
    weight = np.where((fold == 0) | (fold == 16), 1.0, 2.0)
    cosine = weight[None, :] * np.cos(2 * np.pi * freq[:, None] * fold[None, :] / 32)
    modes = np.zeros((NK, QPAD))
    modes[:, :NQ] = np.kron(cosine, cosine)
    return np.concatenate(two_parts(basis), axis=1), *two_parts(modes)


def iota(shape, dim):
    return lax.broadcasted_iota(jnp.int32, shape, dim)


def one_hot(mask):
    return jnp.where(mask, 1.0, 0.0).astype(F32)


def dot(a, b, ca=1, cb=0, precision=None):
    return lax.dot_general(
        a, b, (((ca,), (cb,)), ((), ())), precision=precision, preferred_element_type=F32
    )


def split(v):
    high = v.astype(BF16)
    return high, (v - high.astype(F32)).astype(BF16)


def fold(v, *shifts):
    for shift in shifts:
        v = v + pltpu.roll(v, shift, 1)
    return v


def kernel(
    pe_hbm, cond_hbm, val_hbm, coul_hbm, en_hbm, vec_hbm, kc_hbm, q2_hbm, scr_hbm, mhi_hbm, mlo_hbm,
    out_ref, alpha_ref,
    pe_ref, cond_ref, val_ref, coul_ref, en_ref, vec_ref, kc_ref, q2_ref,
    v8, pairs, lk, pk, coulexp, c8,
    p_out, p_in, q_out, q_in, d_out, d_in, e_out, e_in, f_out, f_in,
    k_out, k_in, h_out, h_in, c16,
    z_out, z_in, y_out, y_in, a_out, a_in, b_out, b_in,
    arow, brow, tt_hi, tt_lo, lam, wt, perm_f, perm_b, scr, m_hi, m_lo,
    send_sems, recv_sems, local_sems,
):
    r, c = lax.axis_index("row"), lax.axis_index("col")
    sizes = {"row": (NR, r), "col": (NC, c)}

    def peers(axis, body):
        size, me = sizes[axis]
        half = size // 2

        def step(i, carry):
            ahead = jnp.where(i < half, half + i, i - half + 1)
            body(lax.rem(me + ahead, size))
            return carry

        lax.fori_loop(0, size - 1, step, 0)

    def send(axis, which, source, target):
        me = sizes[axis][1]

        def one(peer):
            pltpu.make_async_remote_copy(
                src_ref=source(peer),
                dst_ref=target.at[me],
                send_sem=send_sems.at[which],
                recv_sem=recv_sems.at[which],
                device_id={axis: peer},
                device_id_type=MESH,
            ).start()

        peers(axis, one)

    def wait_all(axis, sems, which, target):
        many = target.at[pl.ds(0, sizes[axis][0] - 1)]
        pltpu.make_async_copy(many, many, sems.at[which]).wait()

    def arrived(axis, which, target):
        wait_all(axis, recv_sems, which, target)

    barrier = pltpu.get_barrier_semaphore()
    for axis in ("row", "col"):
        peers(
            axis,
            lambda peer, axis=axis: pl.semaphore_signal(
                barrier, inc=1, device_id={axis: peer}, device_id_type=MESH
            ),
        )
    near = pl.multiple_of((r // 8) * 128, 128)
    far = pl.multiple_of((r // 8) * 128 + 512, 128)
    fetches = [
        pltpu.make_async_copy(source, target, local_sems.at[i])
        for i, (source, target) in enumerate(
            (
                (vec_hbm, vec_ref),
                (cond_hbm, cond_ref),
                (val_hbm, val_ref),
                (kc_hbm, kc_ref),
                (pe_hbm, pe_ref),
                (coul_hbm, coul_ref),
                (en_hbm, en_ref),
                (q2_hbm, q2_ref),
                (scr_hbm.at[:, pl.ds(near, 128)], scr.at[0, pl.ds(0, NQ), :]),
                (scr_hbm.at[:, pl.ds(far, 128)], scr.at[1, pl.ds(0, NQ), :]),
                (mhi_hbm, m_hi),
                (mlo_hbm, m_lo),
            )
        )
    ]
    for fetch in fetches:
        fetch.start()
    for fetch in fetches[:3]:
        fetch.wait()

    vec = vec_ref[...].astype(F32)
    for i in range(8):
        v8[i : i + 1, :] = vec[i // 4 : i // 4 + 1, (i % 4) * 128 : (i % 4 + 1) * 128]
    row32, lane32 = iota((32, 128), 0), iota((32, 128), 1)
    lane_is_t = (row32 & 3) == (lane32 >> 5)
    spread = one_hot((iota((32, 8), 0) >> 2) == iota((32, 8), 1))
    gather8 = one_hot((iota((8, 32), 1) >> 2) == iota((8, 32), 0))
    wide = dot(spread.astype(BF16), v8[...].astype(BF16))
    x128 = fold(jnp.where(lane_is_t, wide, 0.0), 64, 32)

    for k in range(2):
        cond = cond_ref[k].astype(F32)
        val = val_ref[k].astype(F32)
        for v in range(4):
            at = 16 * k + 4 * v
            pairs[at : at + 4, :] = val[v : v + 1, :] * cond
    pair_rows = pairs[...].astype(BF16)
    lk[0:32, :] = pair_rows[:, :512]
    lk[32:64, :] = pair_rows[:, 512:]
    row64, lane64 = iota((64, 128), 0), iota((64, 128), 1)
    own64 = ((row64 >> 5) == ((lane64 >> 5) & 1)) & (((row64 >> 4) & 1) == (lane64 >> 6))
    x_block = jnp.where(own64, jnp.concatenate([x128, x128], axis=0), 0.0).astype(BF16)
    p_out[...] = dot(lk[...], x_block, 0, 0).astype(BF16).reshape(NR, NC, 128)

    pl.semaphore_wait(barrier, NR + NC - 2)
    send("row", X_PROJ_ROW, lambda peer: p_out.at[peer], p_in)
    p_in[pl.ds(r, 1)] = p_out[pl.ds(r, 1)]

    for fetch in fetches[3:]:
        fetch.wait()
    place = iota((1, 128), 1) - 4 * r
    k_row = jnp.zeros((1, 128), jnp.int32)
    for q in range(4):
        k_row = jnp.where(place == q, kc_ref[q // 2, q % 2], k_row)
    k_out[...] = k_row.astype(F32)

    send("row", X_COORD_ROW, lambda peer: k_out, k_in)
    k_in[pl.ds(r, 1)] = k_out[...].reshape(1, 1, 128)

    for k in range(2):
        for j in range(4):
            at = 32 * j + 16 * k
            pk[at : at + 16, :] = pe_ref[k, :, j * 256 : (j + 1) * 256]
    own128 = (iota((128, 128), 0) >> 5) == (iota((128, 128), 1) >> 5)
    x_quarter = jnp.where(own128, jnp.concatenate([x128] * 4, axis=0), 0.0).astype(BF16)
    d_out[...] = dot(pk[...], x_quarter, 0, 0).reshape(NR, 8, 128)

    send("row", X_DENS_ROW, lambda peer: d_out.at[peer], d_in)
    d_in[pl.ds(r, 1)] = d_out[pl.ds(r, 1)]

    def build_perm(i, carry):
        at = pl.multiple_of(i * 128, 128)
        row, col = iota((128, 512), 0) + i * 128, iota((128, 512), 1)
        perm_f[pl.ds(at, 128), :] = one_hot(col == ((row & 31) << 4) + (row >> 5)).astype(BF16)
        perm_b[pl.ds(at, 128), :] = one_hot(col == ((row & 15) << 5) + (row >> 4)).astype(BF16)
        return carry

    lax.fori_loop(0, 4, build_perm, 0)
    c8[...] = jnp.zeros((8, 256), F32)
    for j in range(4):
        c8[j : j + 1, :] = coul_ref[:, j * 256 : (j + 1) * 256]
    expand8 = one_hot(iota((8, 128), 0) == (iota((8, 128), 1) >> 5))
    coulexp[...] = dot(c8[...], expand8, 0, 0, precision=HIGH)

    energy = jnp.concatenate(
        [jnp.broadcast_to(en_ref[k : k + 1, :], (16, 16)) for k in range(2)], axis=0
    )
    same = (iota((32, 16), 0) & 15) == iota((32, 16), 1)
    e_col = jnp.sum(jnp.where(same, energy, 0.0), axis=1, keepdims=True)
    ex128 = e_col * x128
    alpha_energy = dot(x128, ex128, 0, 0, precision=HIGH)[:32]

    arrived("row", X_COORD_ROW, k_in)
    h_out[...] = jnp.sum(k_in[...], axis=0)
    send("col", X_COORD_COL, lambda peer: h_out, h_in)
    h_in[pl.ds(c, 1)] = h_out[...].reshape(1, 1, 128)

    chosen = (r % 8) * 16 + c
    seen = (iota((QPAD, 128), 0) < NQ) & (iota((QPAD, 128), 1) == chosen)
    columns = [jnp.sum(jnp.where(seen, scr[h], 0.0), axis=1, keepdims=True) for h in range(2)]
    lane_q = iota((QPAD, 128), 1)
    s_hi, s_lo = split(jnp.where(((lane_q >> 5) & 1) == 0, columns[0], columns[1]))

    def build_lam(i, carry):
        at = pl.multiple_of(i * 256, 256)
        high, low = m_hi[pl.ds(at, 256), :], m_lo[pl.ds(at, 256), :]
        lam[pl.ds(at, 256), :] = dot(high, s_hi) + dot(high, s_lo) + dot(low, s_hi)
        return carry

    lax.fori_loop(0, 4, build_lam, 0)

    arrived("row", X_PROJ_ROW, p_in)
    mixed = dot(perm_f[...], p_in[...].reshape(512, 128)).astype(BF16)
    q_out[...] = mixed.reshape(NC, NR, 128)
    send("col", X_PROJ_COL, lambda peer: q_out.at[peer], q_in)
    q_in[pl.ds(c, 1)] = q_out[pl.ds(c, 1)]
    arrived("row", X_DENS_ROW, d_in)
    e_out[...] = jnp.sum(d_in[...], axis=0)
    send("col", X_DENS_COL, lambda peer: e_out, e_in)
    e_in[pl.ds(c, 1)] = e_out[...].reshape(1, 8, 128)

    arrived("col", X_COORD_COL, h_in)
    for i in range(NC):
        c16[i : i + 1, :] = h_in[i]
    repeat = one_hot(iota((16, 512), 0) == (iota((16, 512), 1) >> 5)).astype(BF16)
    spread_c = dot(c16[...].astype(BF16), repeat, 0, 0)
    row128, lane512 = iota((128, 512), 0), iota((128, 512), 1)
    kept = jnp.where((row128 >> 2) == (lane512 & 31), spread_c, 0.0).astype(BF16)
    pick = one_hot((iota((128, 128), 0) >> 5) == (iota((128, 128), 1) & 3)).astype(BF16)
    coords = dot(pick, kept)
    hot = one_hot(coords == (row128 & 31).astype(F32)).astype(BF16)
    q2 = q2_ref[...]
    for k in range(2):
        at = 64 * k
        first, second = hot[at : at + 32], hot[at + 32 : at + 64]
        arow[k] = dot(q2, jnp.concatenate([first, first], axis=0))
        brow[k] = dot(q2, jnp.concatenate([second, second], axis=0))

    def build_basis(j, carry):
        at = pl.multiple_of(j * 32, 32)
        for k in range(2):
            high, low = split(arow[k, pl.ds(j, 1), :] * brow[k])
            tt_hi[k, pl.ds(at, 32), :] = high
            tt_lo[k, pl.ds(at, 32), :] = low
        return carry

    lax.fori_loop(0, 32, build_basis, 0)

    arrived("col", X_PROJ_COL, q_in)
    proj = q_in[...].reshape(512, 128)
    lane256 = iota((256, 128), 1)

    def one_block(i, total):
        at = pl.multiple_of(i * 256, 256)
        parts = [
            dot(tt_hi[k, pl.ds(at, 256), :], proj) + dot(tt_lo[k, pl.ds(at, 256), :], proj)
            for k in range(2)
        ]
        mode = fold(jnp.where(lane256 < 64, parts[0], parts[1]), 64)
        scaled = lam[pl.ds(at, 256), :] * mode
        high, low = split(jnp.transpose(scaled)[:64])
        wt[0:64, pl.ds(at, 256)] = high
        wt[64:128, pl.ds(at, 256)] = low
        return total + dot(mode.astype(BF16), scaled.astype(BF16), 0, 0)

    alpha_direct = lax.fori_loop(0, 4, one_block, jnp.zeros((128, 128), F32))
    for k in range(2):
        both = dot(wt[...], tt_hi[k])
        back = both[:64] + both[64:] + dot(wt[0:64, :], tt_lo[k])
        lam[0:512, 64 * k : 64 * k + 64] = jnp.transpose(back)
    z_out[...] = lam[0:512, :].astype(BF16).reshape(NC, NR, 128)
    send("col", X_POT_COL, lambda peer: z_out.at[peer], z_in)
    z_in[pl.ds(c, 1)] = z_out[pl.ds(c, 1)]

    mine = jnp.where((row64 >> 5) == ((lane64 >> 5) & 1), alpha_direct[:64], 0.0)
    part = alpha_energy - fold(mine[:32] + mine[32:], 32) * (1.0 / NK)
    a_out[...] = dot(gather8, jnp.where(lane_is_t, part, 0.0), precision=HIGH)
    send("row", X_ALPHA_ROW, lambda peer: a_out, a_in)
    a_in[pl.ds(r, 1)] = a_out[...].reshape(1, 8, 128)

    arrived("col", X_DENS_COL, e_in)
    f_out[...] = jnp.sum(e_in[...], axis=0)
    send("row", X_DENS_OUT, lambda peer: f_out, f_in)
    f_in[pl.ds(r, 1)] = f_out[...].reshape(1, 8, 128)

    arrived("col", X_POT_COL, z_in)
    mixed = dot(perm_b[...], z_in[...].reshape(512, 128)).astype(BF16)
    y_out[...] = mixed.reshape(NR, NC, 128)
    send("row", X_POT_ROW, lambda peer: y_out.at[peer], y_in)
    y_in[pl.ds(r, 1)] = y_out[pl.ds(r, 1)]
    arrived("row", X_ALPHA_ROW, a_in)
    b_out[...] = jnp.sum(a_in[...], axis=0)
    send("col", X_ALPHA_COL, lambda peer: b_out, b_in)
    b_in[pl.ds(c, 1)] = b_out[...].reshape(1, 8, 128)

    arrived("row", X_DENS_OUT, f_in)
    density = f_in[...].reshape(256, 128)
    weighted = coulexp[...] * density
    w_hi, w_lo = split(weighted)
    quarters = pk[...]

    def total_of(v):
        v = jnp.where(own128, v, 0.0)
        return fold(v[0:32] + v[32:64] + v[64:96] + v[96:128], 64, 32)

    exchange = total_of(dot(quarters, w_hi) + dot(quarters, w_lo))
    alpha_exchange = total_of(dot(density, weighted, 0, 0, precision=HIGH))

    arrived("col", X_ALPHA_COL, b_in)
    shares = dot(spread, jnp.sum(b_in[...], axis=0), precision=HIGH)
    shares = fold(jnp.where(lane_is_t, shares, 0.0), 64, 32)
    alpha = (shares + (2.0 / NT) * alpha_exchange) * (1.0 / NT)
    alpha_ref[...] = alpha[:, :32]
    base = ex128 + (2.0 / NT) * exchange - dot(x128[:, :32], alpha, precision=HIGH)

    arrived("row", X_POT_ROW, y_in)
    direct = jnp.where(own64, dot(lk[...], y_in[...].reshape(512, 128)), 0.0)
    residual = base - fold(direct[:32] + direct[32:], 64, 32) * (1.0 / NK)
    rows = dot(gather8, jnp.where(lane_is_t, residual, 0.0), precision=HIGH)
    for i in range(8):
        out_ref[i // 4 : i // 4 + 1, (i % 4) * 128 : (i % 4 + 1) * 128] = rows[i : i + 1, :]

    for axis, which, target in (
        ("row", X_COORD_ROW, k_in),
        ("row", X_PROJ_ROW, p_in),
        ("row", X_DENS_ROW, d_in),
        ("col", X_COORD_COL, h_in),
        ("col", X_PROJ_COL, q_in),
        ("col", X_DENS_COL, e_in),
        ("row", X_DENS_OUT, f_in),
        ("col", X_POT_COL, z_in),
        ("row", X_POT_ROW, y_in),
        ("row", X_ALPHA_ROW, a_in),
        ("col", X_ALPHA_COL, b_in),
    ):
        wait_all(axis, send_sems, which, target)


def on_device(pair_exchange, conduction, valence, coulomb, screening, energies, vectors, k_coords):
    q2, m_hi, m_lo = (jnp.asarray(table) for table in tables())
    operands = (
        *(pair_exchange, conduction, valence, coulomb.reshape(1, -1), energies, vectors, k_coords),
        *(q2, screening, m_hi, m_lo),
    )
    vmem = pl.BlockSpec(memory_space=pltpu.VMEM)
    return pl.pallas_call(
        kernel,
        out_shape=(
            jax.ShapeDtypeStruct((2, 512), F32),
            jax.ShapeDtypeStruct((32, 32), F32),
        ),
        in_specs=[pl.BlockSpec(memory_space=pltpu.HBM)] * 11,
        out_specs=(vmem, vmem),
        scratch_shapes=[
            pltpu.VMEM((2, 16, 1024), BF16),
            pltpu.VMEM((2, 4, 1024), BF16),
            pltpu.VMEM((2, 4, 1024), BF16),
            pltpu.VMEM((1, 1024), F32),
            pltpu.VMEM((2, 16), F32),
            pltpu.VMEM((2, 512), BF16),
            pltpu.SMEM((2, 2), jnp.int32),
            pltpu.VMEM((32, 64), BF16),
            pltpu.VMEM((8, 128), F32),
            pltpu.VMEM((32, 1024), F32),
            pltpu.VMEM((64, 512), BF16),
            pltpu.VMEM((128, 256), BF16),
            pltpu.VMEM((256, 128), F32),
            pltpu.VMEM((8, 256), F32),
            pltpu.VMEM((NR, NC, 128), BF16),
            pltpu.VMEM((NR, NC, 128), BF16),
            pltpu.VMEM((NC, NR, 128), BF16),
            pltpu.VMEM((NC, NR, 128), BF16),
            pltpu.VMEM((NR, 8, 128), F32),
            pltpu.VMEM((NR, 8, 128), F32),
            pltpu.VMEM((8, 128), F32),
            pltpu.VMEM((NC, 8, 128), F32),
            pltpu.VMEM((8, 128), F32),
            pltpu.VMEM((NR, 8, 128), F32),
            pltpu.VMEM((1, 128), F32),
            pltpu.VMEM((NR, 1, 128), F32),
            pltpu.VMEM((1, 128), F32),
            pltpu.VMEM((NC, 1, 128), F32),
            pltpu.VMEM((16, 128), F32),
            pltpu.VMEM((NC, NR, 128), BF16),
            pltpu.VMEM((NC, NR, 128), BF16),
            pltpu.VMEM((NR, NC, 128), BF16),
            pltpu.VMEM((NR, NC, 128), BF16),
            pltpu.VMEM((8, 128), F32),
            pltpu.VMEM((NR, 8, 128), F32),
            pltpu.VMEM((8, 128), F32),
            pltpu.VMEM((NC, 8, 128), F32),
            pltpu.VMEM((2, 32, 512), F32),
            pltpu.VMEM((2, 32, 512), F32),
            pltpu.VMEM((2, NK, 512), BF16),
            pltpu.VMEM((2, NK, 512), BF16),
            pltpu.VMEM((NK, 128), F32),
            pltpu.VMEM((128, NK), BF16),
            pltpu.VMEM((512, 512), BF16),
            pltpu.VMEM((512, 512), BF16),
            pltpu.VMEM((2, QPAD, 128), F32),
            pltpu.VMEM((NK, QPAD), BF16),
            pltpu.VMEM((NK, QPAD), BF16),
            pltpu.SemaphoreType.DMA((11,)),
            pltpu.SemaphoreType.DMA((11,)),
            pltpu.SemaphoreType.DMA((12,)),
        ],
        compiler_params=pltpu.CompilerParams(
            collective_id=0, has_side_effects=True, vmem_limit_bytes=24 * 1024 * 1024
        ),
    )(*(pltpu.with_memory_space_constraint(v, pltpu.HBM) for v in operands))


def solution(mesh):
    split_k = ("row", "col")
    return jax.shard_map(
        on_device,
        mesh=mesh,
        in_specs=(
            P(split_k, None, None),
            P(split_k, None, None),
            P(split_k, None, None),
            P(),
            P(),
            P(split_k, None),
            P(split_k, None),
            P(split_k, None),
        ),
        out_specs=(P(split_k, None), P()),
        check_vma=False,
    )
```

```python
import jax
import jax.numpy as jnp
import numpy as np
from jax import lax
from jax.experimental import pallas as pl
from jax.experimental.pallas import tpu as pltpu
from jax.sharding import PartitionSpec as P

MESH = pl.DeviceIdType.MESH
HIGH = lax.Precision.HIGHEST
F32 = jnp.float32
BF16 = jnp.bfloat16

NR, NC, NU = 32, 16, 16
NK, NT = 1024, 16384
NQ = 289
QPAD = 384
COORD_ROW, COORD_COL, PROJ_ROW, PROJ_COL, POT_COL, POT_ROW = range(6)
DENS_PAIR, DENS_ROW, DENS_COL, DENS_OUT, DENS_SWAP = range(6, 11)
ALPHA_PAIR, ALPHA_ROW, ALPHA_COL, ALPHA_SWAP = range(11, 15)


def real_basis():
    points = np.arange(32)[None, :]
    order = np.arange(32)[:, None]
    freq = np.where(order <= 16, order, order - 16)
    angle = 2 * np.pi * freq * points / 32
    basis = np.where(order <= 16, np.cos(angle), np.sin(angle)) * np.sqrt(2 / 32)
    basis[[0, 16]] *= np.sqrt(0.5)
    return basis, freq[:, 0]


def two_parts(table):
    high = table.astype(BF16)
    return high, (table - high.astype(np.float64)).astype(BF16)


def tables():
    basis, freq = real_basis()
    fold = np.arange(17)
    weight = np.where((fold == 0) | (fold == 16), 1.0, 2.0)
    cosine = weight[None, :] * np.cos(2 * np.pi * freq[:, None] * fold[None, :] / 32)
    modes = np.zeros((QPAD, NK))
    modes[:NQ] = np.kron(cosine, cosine).T
    narrow = np.concatenate(two_parts(basis), axis=1)
    outer = np.concatenate(two_parts(np.repeat(basis.T, 32, axis=1)), axis=0)
    inner = np.concatenate(two_parts(np.tile(basis.T, (1, 32))), axis=0)
    return narrow, outer, inner, *two_parts(modes)


def iota(shape, dim):
    return lax.broadcasted_iota(jnp.int32, shape, dim)


def one_hot(mask):
    return jnp.where(mask, 1.0, 0.0).astype(F32)


def dot(a, b, ca=1, cb=0, precision=None):
    return lax.dot_general(
        a, b, (((ca,), (cb,)), ((), ())), precision=precision, preferred_element_type=F32
    )


def split(v):
    high = v.astype(BF16)
    return high, (v - high.astype(F32)).astype(BF16)


def fold(v, *shifts):
    for shift in shifts:
        v = v + pltpu.roll(v, shift, 1)
    return v


def kernel(
    pe_hbm, cond_hbm, val_hbm, coul_hbm, en_hbm, vec_hbm, kc_hbm, q2_hbm, qa_hbm, qb_hbm, scr_hbm,
    mhi_hbm, mlo_hbm,
    out_ref, alpha_ref,
    pe_ref, cond_ref, val_ref, coul_ref, en_ref, vec_ref, kc_ref, q2_ref, qa_ref, qb_ref,
    v8, pairs, lk, pk, coulexp, c8,
    p_out, p_in, q_out, q_in, z_out, z_in, y_out, y_in,
    k_out, k_in, h_out, h_in, c16,
    d_out, d_pair, d_sum, d_in, e_out, e_in, f_out, f_in,
    a_out, a_pair, b_out, b_in, g_out, g_in, a_full,
    arow, brow, t_all, tt_hi, tt_lo, lam, wt, z_wide, perm_f, perm_b, scr, m_hi, m_lo,
    send_sems, recv_sems, local_sems,
):
    r, c = lax.axis_index("row"), lax.axis_index("col")
    core, chip = lax.rem(r, 2), r // 2
    groups = {"row": (NR, r), "col": (NC, c), "chip": (NU, chip)}

    def device(group, peer):
        if group == "chip":
            return {"row": 2 * peer + core}
        return {group: peer}

    def peers(group, body):
        size, me = groups[group]
        half = size // 2

        def step(i, carry):
            ahead = jnp.where(i < half, half + i, i - half + 1)
            body(lax.rem(me + ahead, size))
            return carry

        lax.fori_loop(0, size - 1, step, 0)

    def copy_to(device_id, which, source, target):
        return pltpu.make_async_remote_copy(
            src_ref=source,
            dst_ref=target,
            send_sem=send_sems.at[which],
            recv_sem=recv_sems.at[which],
            device_id=device_id,
            device_id_type=MESH,
        )

    def send(group, which, source, target, base=0):
        slot = base + groups[group][1]
        peers(
            group,
            lambda peer: copy_to(
                device(group, peer), which, source(peer), target.at[slot]
            ).start(),
        )

    def wait_bytes(sem, many):
        pltpu.make_async_copy(many, many, sem).wait()

    waits = []

    def arrived(group, which, target):
        many = target.at[pl.ds(0, groups[group][0] - 1)]
        waits.append((which, many))
        wait_bytes(recv_sems.at[which], many)

    def arrived_pair(which, target):
        waits.append((which, target))
        wait_bytes(recv_sems.at[which], target)

    sibling = {"row": r + 1 - 2 * core}

    barrier = pltpu.get_barrier_semaphore()
    for axis in ("row", "col"):
        peers(
            axis,
            lambda peer, axis=axis: pl.semaphore_signal(
                barrier, inc=1, device_id={axis: peer}, device_id_type=MESH
            ),
        )
    near = pl.multiple_of((r // 8) * 128, 128)
    far = pl.multiple_of((r // 8) * 128 + 512, 128)
    fetches = [
        pltpu.make_async_copy(source, target, local_sems.at[i])
        for i, (source, target) in enumerate(
            (
                (vec_hbm, vec_ref),
                (cond_hbm, cond_ref),
                (val_hbm, val_ref),
                (kc_hbm, kc_ref),
                (pe_hbm, pe_ref),
                (coul_hbm, coul_ref),
                (en_hbm, en_ref),
                (q2_hbm, q2_ref),
                (scr_hbm.at[:, pl.ds(near, 128)], scr.at[0, pl.ds(0, NQ), :]),
                (scr_hbm.at[:, pl.ds(far, 128)], scr.at[1, pl.ds(0, NQ), :]),
                (mhi_hbm, m_hi),
                (mlo_hbm, m_lo),
                (qa_hbm, qa_ref),
                (qb_hbm, qb_ref),
            )
        )
    ]
    for fetch in fetches:
        fetch.start()
    for fetch in fetches[:3]:
        fetch.wait()

    vec = vec_ref[...].astype(F32)
    for i in range(8):
        v8[i : i + 1, :] = vec[i // 4 : i // 4 + 1, (i % 4) * 128 : (i % 4 + 1) * 128]
    row32, lane32 = iota((32, 128), 0), iota((32, 128), 1)
    lane_is_t = (row32 & 3) == (lane32 >> 5)
    spread = one_hot((iota((32, 8), 0) >> 2) == iota((32, 8), 1))
    gather8 = one_hot((iota((8, 32), 1) >> 2) == iota((8, 32), 0))
    wide = dot(spread.astype(BF16), v8[...].astype(BF16))
    x128 = fold(jnp.where(lane_is_t, wide, 0.0), 64, 32)

    for k in range(2):
        cond = cond_ref[k].astype(F32)
        val = val_ref[k].astype(F32)
        for v in range(4):
            at = 16 * k + 4 * v
            pairs[at : at + 4, :] = val[v : v + 1, :] * cond
    pair_rows = pairs[...].astype(BF16)
    lk[0:32, :] = pair_rows[:, :512]
    lk[32:64, :] = pair_rows[:, 512:]
    row64, lane64 = iota((64, 128), 0), iota((64, 128), 1)
    own64 = ((row64 >> 5) == ((lane64 >> 5) & 1)) & (((row64 >> 4) & 1) == (lane64 >> 6))
    x_block = jnp.where(own64, jnp.concatenate([x128, x128], axis=0), 0.0).astype(BF16)
    p_out[...] = dot(lk[...], x_block, 0, 0).astype(BF16).reshape(NR, NC, 128)

    for fetch in fetches[3:8]:
        fetch.wait()
    place = iota((1, 128), 1) - 4 * r
    k_row = jnp.zeros((1, 128), jnp.int32)
    for q in range(4):
        k_row = jnp.where(place == q, kc_ref[q // 2, q % 2], k_row)
    k_out[...] = k_row.astype(F32)

    pl.semaphore_wait(barrier, NR + NC - 2)
    send("row", COORD_ROW, lambda peer: k_out, k_in)
    send("row", PROJ_ROW, lambda peer: p_out.at[peer], p_in)
    k_in[pl.ds(r, 1)] = k_out[...].reshape(1, 1, 128)
    p_in[pl.ds(r, 1)] = p_out[pl.ds(r, 1)]

    for k in range(2):
        for j in range(4):
            at = 32 * j + 16 * k
            pk[at : at + 16, :] = pe_ref[k, :, j * 256 : (j + 1) * 256]
    own128 = (iota((128, 128), 0) >> 5) == (iota((128, 128), 1) >> 5)
    x_quarter = jnp.where(own128, jnp.concatenate([x128] * 4, axis=0), 0.0).astype(BF16)
    d_out[...] = dot(pk[...], x_quarter, 0, 0).reshape(NR, 8, 128)
    mine = pl.multiple_of(core * NU, NU)
    other = pl.multiple_of(NU - core * NU, NU)
    copy_to(sibling, DENS_PAIR, d_out.at[pl.ds(other, NU)], d_pair).start()

    def build_perm(i, carry):
        at = pl.multiple_of(i * 128, 128)
        row, col = iota((128, 512), 0) + i * 128, iota((128, 512), 1)
        perm_f[pl.ds(at, 128), :] = one_hot(col == ((row & 31) << 4) + (row >> 5)).astype(BF16)
        perm_b[pl.ds(at, 128), :] = one_hot(col == ((row & 15) << 5) + (row >> 4)).astype(BF16)
        return carry

    lax.fori_loop(0, 4, build_perm, 0)

    arrived_pair(DENS_PAIR, d_pair)
    d_sum[...] = d_out[pl.ds(mine, NU)] + d_pair[...]
    send("chip", DENS_ROW, lambda peer: d_sum.at[peer], d_in)
    d_in[pl.ds(chip, 1)] = d_sum[pl.ds(chip, 1)]

    for fetch in fetches[8:]:
        fetch.wait()
    chosen = lax.rem(r, 8) * 16 + c
    q_row, q_lane = iota((8, 128), 0), iota((8, 128), 1)
    known = iota((QPAD, 128), 0) < NQ
    values = sum(
        dot(
            one_hot((q_row == h) & (q_lane == chosen)),
            jnp.where(known, scr[h], 0.0),
            1,
            1,
            precision=HIGH,
        )
        for h in range(2)
    )
    s_hi, s_lo = split(values)
    lam[...] = dot(s_hi, m_hi[...]) + dot(s_lo, m_hi[...]) + dot(s_hi, m_lo[...])

    arrived("row", COORD_ROW, k_in)
    h_out[...] = jnp.sum(k_in[...], axis=0)
    send("col", COORD_COL, lambda peer: h_out, h_in)
    h_in[pl.ds(c, 1)] = h_out[...].reshape(1, 1, 128)

    arrived("row", PROJ_ROW, p_in)
    mixed = dot(perm_f[...], p_in[...].reshape(512, 128)).astype(BF16)
    q_out[...] = mixed.reshape(NC, NR, 128)
    send("col", PROJ_COL, lambda peer: q_out.at[peer], q_in)
    q_in[pl.ds(c, 1)] = q_out[pl.ds(c, 1)]
    arrived("chip", DENS_ROW, d_in)
    e_out[...] = jnp.sum(d_in[...], axis=0)
    send("col", DENS_COL, lambda peer: e_out, e_in)
    e_in[pl.ds(c, 1)] = e_out[...].reshape(1, 8, 128)

    arrived("col", COORD_COL, h_in)
    for i in range(NC):
        c16[i : i + 1, :] = h_in[i]
    repeat = one_hot(iota((16, 512), 0) == (iota((16, 512), 1) >> 5)).astype(BF16)
    spread_c = dot(c16[...].astype(BF16), repeat, 0, 0)
    row128, lane512 = iota((128, 512), 0), iota((128, 512), 1)
    kept = jnp.where((row128 >> 2) == (lane512 & 31), spread_c, 0.0).astype(BF16)
    pick = one_hot((iota((128, 128), 0) >> 5) == (iota((128, 128), 1) & 3)).astype(BF16)
    coords = dot(pick, kept)
    hot = one_hot(coords == (row128 & 31).astype(F32)).astype(BF16)
    q2 = q2_ref[...]
    for k in range(2):
        at = 64 * k
        first = jnp.concatenate([hot[at : at + 32]] * 2, axis=0)
        second = jnp.concatenate([hot[at + 32 : at + 64]] * 2, axis=0)
        arow[k] = dot(q2, first)
        brow[k] = dot(q2, second)
        for i in range(4):
            at = 128 * i
            outer = dot(first[:, at : at + 128], qa_ref[...], 0, 0)
            inner = dot(second[:, at : at + 128], qb_ref[...], 0, 0)
            high, low = split(outer * inner)
            t_all[512 * k + at : 512 * k + at + 128, :] = high
            t_all[1024 + 512 * k + at : 1024 + 512 * k + at + 128, :] = low

    def build_basis(j, carry):
        at = pl.multiple_of(j * 32, 32)
        for k in range(2):
            high, low = split(arow[k, pl.ds(j, 1), :] * brow[k])
            tt_hi[k, pl.ds(at, 32), :] = high
            tt_lo[k, pl.ds(at, 32), :] = low
        return carry

    lax.fori_loop(0, 32, build_basis, 0)

    arrived("col", PROJ_COL, q_in)
    turned = jnp.transpose(q_in[...].reshape(512, 128).astype(F32)).astype(BF16)
    mode = dot(jnp.concatenate([turned[:64], turned[64:]] * 2, axis=1), t_all[...])
    first_g = iota((64, NK), 0) < 32
    scaled = jnp.where(first_g, lam[0:1, :], lam[1:2, :]) * mode
    high, low = split(scaled)
    wt[0:64, :] = high
    wt[64:128, :] = low
    for k in range(2):
        both = dot(wt[...], tt_hi[k])
        back = both[:64] + both[64:] + dot(wt[0:64, :], tt_lo[k])
        z_wide[64 * k : 64 * k + 64, :] = back
    z_out[...] = jnp.transpose(z_wide[...]).astype(BF16).reshape(NC, NR, 128)
    send("col", POT_COL, lambda peer: z_out.at[peer], z_in)
    z_in[pl.ds(c, 1)] = z_out[pl.ds(c, 1)]

    energy = jnp.concatenate(
        [jnp.broadcast_to(en_ref[k : k + 1, :], (16, 16)) for k in range(2)], axis=0
    )
    same = (iota((32, 16), 0) & 15) == iota((32, 16), 1)
    e_col = jnp.sum(jnp.where(same, energy, 0.0), axis=1, keepdims=True)
    ex128 = e_col * x128
    alpha_energy = dot(x128, ex128, 0, 0, precision=HIGH)[:32]
    alpha_direct = dot(mode.astype(BF16), jnp.concatenate([high, high], axis=0), 1, 1)
    kept_g = jnp.where((row64 >> 5) == ((lane64 >> 5) & 1), alpha_direct, 0.0)
    part = alpha_energy - fold(kept_g[:32] + kept_g[32:], 32) * (1.0 / NK)
    packed = dot(gather8, jnp.where(lane_is_t, part, 0.0), precision=HIGH)
    a_out[0] = packed[0:4]
    a_out[1] = packed[4:8]
    copy_to(sibling, ALPHA_PAIR, a_out.at[1 - core], a_pair.at[0]).start()

    arrived("col", DENS_COL, e_in)
    f_out[...] = jnp.sum(e_in[...], axis=0)
    send("chip", DENS_OUT, lambda peer: f_out, f_in, base=mine)
    f_in[pl.ds(mine + chip, 1)] = f_out[...].reshape(1, 8, 128)

    arrived_pair(ALPHA_PAIR, a_pair)
    b_out[...] = a_out[pl.ds(core, 1)] + a_pair[...]
    send("chip", ALPHA_ROW, lambda peer: b_out.at[0], b_in)
    b_in[pl.ds(chip, 1)] = b_out[...]

    c8[...] = jnp.zeros((8, 256), F32)
    for j in range(4):
        c8[j : j + 1, :] = coul_ref[:, j * 256 : (j + 1) * 256]
    expand8 = one_hot(iota((8, 128), 0) == (iota((8, 128), 1) >> 5))
    coulexp[...] = dot(c8[...], expand8, 0, 0, precision=HIGH)

    arrived("col", POT_COL, z_in)
    mixed = dot(perm_b[...], z_in[...].reshape(512, 128)).astype(BF16)
    y_out[...] = mixed.reshape(NR, NC, 128)
    send("row", POT_ROW, lambda peer: y_out.at[peer], y_in)
    y_in[pl.ds(r, 1)] = y_out[pl.ds(r, 1)]

    arrived("chip", ALPHA_ROW, b_in)
    g_out[...] = jnp.sum(b_in[...], axis=0, keepdims=True)
    send("col", ALPHA_COL, lambda peer: g_out.at[0], g_in)
    g_in[pl.ds(c, 1)] = g_out[...]

    arrived("chip", DENS_OUT, f_in)
    half = f_in.at[pl.ds(mine, NU)]
    copy_to(sibling, DENS_SWAP, half, half).start()
    arrived_pair(DENS_SWAP, f_in.at[pl.ds(other, NU)])
    density = f_in[...].reshape(256, 128)
    weighted = coulexp[...] * density
    w_hi, w_lo = split(weighted)
    quarters = pk[...]

    def total_of(v):
        v = jnp.where(own128, v, 0.0)
        return fold(v[0:32] + v[32:64] + v[64:96] + v[96:128], 64, 32)

    exchange = total_of(dot(quarters, w_hi) + dot(quarters, w_lo))
    alpha_exchange = total_of(dot(density, weighted, 0, 0, precision=HIGH))

    arrived("col", ALPHA_COL, g_in)
    a_full[pl.ds(core, 1)] = jnp.sum(g_in[...], axis=0, keepdims=True)
    copy_to(sibling, ALPHA_SWAP, a_full.at[core], a_full.at[core]).start()
    arrived_pair(ALPHA_SWAP, a_full.at[1 - core])
    shares = dot(spread[:, 0:4], a_full[0], precision=HIGH)
    shares = shares + dot(spread[:, 4:8], a_full[1], precision=HIGH)
    shares = fold(jnp.where(lane_is_t, shares, 0.0), 64, 32)
    alpha = (shares + (2.0 / NT) * alpha_exchange) * (1.0 / NT)
    alpha_ref[...] = alpha[:, :32]
    base = ex128 + (2.0 / NT) * exchange - dot(x128[:, :32], alpha, precision=HIGH)

    arrived("row", POT_ROW, y_in)
    direct = jnp.where(own64, dot(lk[...], y_in[...].reshape(512, 128)), 0.0)
    residual = base - fold(direct[:32] + direct[32:], 64, 32) * (1.0 / NK)
    rows = dot(gather8, jnp.where(lane_is_t, residual, 0.0), precision=HIGH)
    for i in range(8):
        out_ref[i // 4 : i // 4 + 1, (i % 4) * 128 : (i % 4 + 1) * 128] = rows[i : i + 1, :]

    for which, many in waits:
        wait_bytes(send_sems.at[which], many)


def on_device(pair_exchange, conduction, valence, coulomb, screening, energies, vectors, k_coords):
    q2, qa, qb, m_hi, m_lo = (jnp.asarray(table) for table in tables())
    operands = (
        *(pair_exchange, conduction, valence, coulomb.reshape(1, -1), energies, vectors, k_coords),
        *(q2, qa, qb, screening, m_hi, m_lo),
    )
    vmem = pl.BlockSpec(memory_space=pltpu.VMEM)
    return pl.pallas_call(
        kernel,
        out_shape=(
            jax.ShapeDtypeStruct((2, 512), F32),
            jax.ShapeDtypeStruct((32, 32), F32),
        ),
        in_specs=[pl.BlockSpec(memory_space=pltpu.HBM)] * len(operands),
        out_specs=(vmem, vmem),
        scratch_shapes=[
            pltpu.VMEM((2, 16, 1024), BF16),
            pltpu.VMEM((2, 4, 1024), BF16),
            pltpu.VMEM((2, 4, 1024), BF16),
            pltpu.VMEM((1, 1024), F32),
            pltpu.VMEM((2, 16), F32),
            pltpu.VMEM((2, 512), BF16),
            pltpu.SMEM((2, 2), jnp.int32),
            pltpu.VMEM((32, 64), BF16),
            pltpu.VMEM((64, NK), BF16),
            pltpu.VMEM((64, NK), BF16),
            pltpu.VMEM((8, 128), F32),
            pltpu.VMEM((32, 1024), F32),
            pltpu.VMEM((64, 512), BF16),
            pltpu.VMEM((128, 256), BF16),
            pltpu.VMEM((256, 128), F32),
            pltpu.VMEM((8, 256), F32),
            pltpu.VMEM((NR, NC, 128), BF16),
            pltpu.VMEM((NR, NC, 128), BF16),
            pltpu.VMEM((NC, NR, 128), BF16),
            pltpu.VMEM((NC, NR, 128), BF16),
            pltpu.VMEM((NC, NR, 128), BF16),
            pltpu.VMEM((NC, NR, 128), BF16),
            pltpu.VMEM((NR, NC, 128), BF16),
            pltpu.VMEM((NR, NC, 128), BF16),
            pltpu.VMEM((1, 128), F32),
            pltpu.VMEM((NR, 1, 128), F32),
            pltpu.VMEM((1, 128), F32),
            pltpu.VMEM((NC, 1, 128), F32),
            pltpu.VMEM((16, 128), F32),
            pltpu.VMEM((NR, 8, 128), F32),
            pltpu.VMEM((NU, 8, 128), F32),
            pltpu.VMEM((NU, 8, 128), F32),
            pltpu.VMEM((NU, 8, 128), F32),
            pltpu.VMEM((8, 128), F32),
            pltpu.VMEM((NC, 8, 128), F32),
            pltpu.VMEM((8, 128), F32),
            pltpu.VMEM((NR, 8, 128), F32),
            pltpu.VMEM((2, 4, 128), F32),
            pltpu.VMEM((1, 4, 128), F32),
            pltpu.VMEM((1, 4, 128), F32),
            pltpu.VMEM((NU, 4, 128), F32),
            pltpu.VMEM((1, 4, 128), F32),
            pltpu.VMEM((NC, 4, 128), F32),
            pltpu.VMEM((2, 4, 128), F32),
            pltpu.VMEM((2, 32, 512), F32),
            pltpu.VMEM((2, 32, 512), F32),
            pltpu.VMEM((2048, NK), BF16),
            pltpu.VMEM((2, NK, 512), BF16),
            pltpu.VMEM((2, NK, 512), BF16),
            pltpu.VMEM((8, NK), F32),
            pltpu.VMEM((128, NK), BF16),
            pltpu.VMEM((128, 512), F32),
            pltpu.VMEM((512, 512), BF16),
            pltpu.VMEM((512, 512), BF16),
            pltpu.VMEM((2, QPAD, 128), F32),
            pltpu.VMEM((QPAD, NK), BF16),
            pltpu.VMEM((QPAD, NK), BF16),
            pltpu.SemaphoreType.DMA((15,)),
            pltpu.SemaphoreType.DMA((15,)),
            pltpu.SemaphoreType.DMA((14,)),
        ],
        compiler_params=pltpu.CompilerParams(
            collective_id=0, has_side_effects=True, vmem_limit_bytes=32 * 1024 * 1024
        ),
    )(*(pltpu.with_memory_space_constraint(v, pltpu.HBM) for v in operands))


def solution(mesh):
    split_k = ("row", "col")
    return jax.shard_map(
        on_device,
        mesh=mesh,
        in_specs=(
            P(split_k, None, None),
            P(split_k, None, None),
            P(split_k, None, None),
            P(),
            P(),
            P(split_k, None),
            P(split_k, None),
            P(split_k, None),
        ),
        out_specs=(P(split_k, None), P()),
        check_vma=False,
    )
```

```python
import jax
import jax.numpy as jnp
import numpy as np
from jax import lax
from jax.experimental import pallas as pl
from jax.experimental.pallas import tpu as pltpu
from jax.sharding import PartitionSpec as P

MESH = pl.DeviceIdType.MESH
HIGH = lax.Precision.HIGHEST
F32 = jnp.float32
BF16 = jnp.bfloat16

NR, NC, NU = 32, 16, 16
NK, NT = 1024, 16384
NQ = 289
QPAD = 384
COORD_ROW, COORD_COL, PROJ_ROW, PROJ_COL, POT_COL, POT_ROW = range(6)
DENS_PAIR, DENS_ROW, DENS_COL, DENS_OUT, DENS_SWAP = range(6, 11)
ALPHA_ROW, ALPHA_COL = range(11, 13)


def real_basis():
    points = np.arange(32)[None, :]
    order = np.arange(32)[:, None]
    freq = np.where(order <= 16, order, order - 16)
    angle = 2 * np.pi * freq * points / 32
    basis = np.where(order <= 16, np.cos(angle), np.sin(angle)) * np.sqrt(2 / 32)
    basis[[0, 16]] *= np.sqrt(0.5)
    return basis, freq[:, 0]


def two_parts(table):
    high = table.astype(BF16)
    return high, (table - high.astype(np.float64)).astype(BF16)


def tables():
    basis, freq = real_basis()
    fold = np.arange(17)
    weight = np.where((fold == 0) | (fold == 16), 1.0, 2.0)
    cosine = weight[None, :] * np.cos(2 * np.pi * freq[:, None] * fold[None, :] / 32)
    modes = np.zeros((QPAD, NK))
    modes[:NQ] = np.kron(cosine, cosine).T
    narrow = np.concatenate(two_parts(basis), axis=1)
    outer = np.concatenate(two_parts(np.repeat(basis.T, 32, axis=1)), axis=0)
    inner = np.concatenate(two_parts(np.tile(basis.T, (1, 32))), axis=0)
    return narrow, outer, inner, *two_parts(modes)


def iota(shape, dim):
    return lax.broadcasted_iota(jnp.int32, shape, dim)


def one_hot(mask):
    return jnp.where(mask, 1.0, 0.0).astype(F32)


def dot(a, b, ca=1, cb=0, precision=None):
    return lax.dot_general(
        a, b, (((ca,), (cb,)), ((), ())), precision=precision, preferred_element_type=F32
    )


def split(v):
    high = v.astype(BF16)
    return high, (v - high.astype(F32)).astype(BF16)


def fold(v, *shifts):
    for shift in shifts:
        v = v + pltpu.roll(v, shift, 1)
    return v


def kernel(
    pe_hbm, cond_hbm, val_hbm, coul_hbm, en_hbm, vec_hbm, kc_hbm, q2_hbm, qa_hbm, qb_hbm, scr_hbm,
    mhi_hbm, mlo_hbm,
    out_ref, alpha_ref,
    pe_ref, cond_ref, val_ref, coul_ref, en_ref, vec_ref, kc_ref, q2_ref, qa_ref, qb_ref,
    v8, pairs, lk, pk, coulexp, c8,
    p_out, p_in, q_out, q_in, z_out, z_in, y_out, y_in,
    k_out, k_in, h_out, h_in, c16,
    d_out, d_pair, d_sum, d_in, e_out, e_in, f_out, f_in,
    a_out, a_in, b_out, b_in,
    arow, brow, t_all, tt_hi, tt_lo, lam, wt, z_wide, perm_f, perm_b, scr, m_hi, m_lo,
    send_sems, recv_sems, local_sems,
):
    r, c = lax.axis_index("row"), lax.axis_index("col")
    core, chip = lax.rem(r, 2), r // 2
    groups = {"row": (NR, r), "col": (NC, c), "chip": (NU, chip)}

    def device(group, peer):
        if group == "chip":
            return {"row": 2 * peer + core}
        return {group: peer}

    def nth_peer(group, i):
        size, me = groups[group]
        half = size // 2
        return lax.rem(me + jnp.where(i < half, half + i, i - half + 1), size)

    def peers(group, body):
        def step(i, carry):
            body(nth_peer(group, i))
            return carry

        lax.fori_loop(0, groups[group][0] - 1, step, 0)

    def copy_to(device_id, which, source, target):
        return pltpu.make_async_remote_copy(
            src_ref=source,
            dst_ref=target,
            send_sem=send_sems.at[which],
            recv_sem=recv_sems.at[which],
            device_id=device_id,
            device_id_type=MESH,
        )

    def send(group, which, source, target, base=0):
        slot = base + groups[group][1]
        peers(
            group,
            lambda peer: copy_to(
                device(group, peer), which, source(peer), target.at[slot]
            ).start(),
        )

    def wait_bytes(sem, many):
        pltpu.make_async_copy(many, many, sem).wait()

    waits = []

    def arrived(group, which, target):
        many = target.at[pl.ds(0, groups[group][0] - 1)]
        waits.append((which, many))
        wait_bytes(recv_sems.at[which], many)

    def arrived_pair(which, target):
        waits.append((which, target))
        wait_bytes(recv_sems.at[which], target)

    sibling = {"row": r + 1 - 2 * core}

    barrier = pltpu.get_barrier_semaphore()

    def hello(i, carry):
        for axis in ("col", "row"):
            peer = nth_peer(axis, i)
            pl.semaphore_signal(barrier, inc=1, device_id={axis: peer}, device_id_type=MESH)
        return carry

    def hello_row(i, carry):
        peer = nth_peer("row", i)
        pl.semaphore_signal(barrier, inc=1, device_id={"row": peer}, device_id_type=MESH)
        return carry

    lax.fori_loop(0, NC - 1, hello, 0)
    lax.fori_loop(NC - 1, NR - 1, hello_row, 0)
    near = pl.multiple_of((r // 8) * 128, 128)
    far = pl.multiple_of((r // 8) * 128 + 512, 128)
    fetches = [
        pltpu.make_async_copy(source, target, local_sems.at[i])
        for i, (source, target) in enumerate(
            (
                (vec_hbm, vec_ref),
                (cond_hbm, cond_ref),
                (val_hbm, val_ref),
                (kc_hbm, kc_ref),
                (pe_hbm, pe_ref),
                (coul_hbm, coul_ref),
                (en_hbm, en_ref),
                (q2_hbm, q2_ref),
                (scr_hbm.at[:, pl.ds(near, 128)], scr.at[0, pl.ds(0, NQ), :]),
                (scr_hbm.at[:, pl.ds(far, 128)], scr.at[1, pl.ds(0, NQ), :]),
                (mhi_hbm, m_hi),
                (mlo_hbm, m_lo),
                (qa_hbm, qa_ref),
                (qb_hbm, qb_ref),
            )
        )
    ]
    for fetch in fetches:
        fetch.start()
    for fetch in fetches[:3]:
        fetch.wait()

    vec = vec_ref[...].astype(F32)
    for i in range(8):
        v8[i : i + 1, :] = vec[i // 4 : i // 4 + 1, (i % 4) * 128 : (i % 4 + 1) * 128]
    row32, lane32 = iota((32, 128), 0), iota((32, 128), 1)
    lane_is_t = (row32 & 3) == (lane32 >> 5)
    spread = one_hot((iota((32, 8), 0) >> 2) == iota((32, 8), 1))
    gather8 = one_hot((iota((8, 32), 1) >> 2) == iota((8, 32), 0))
    wide = dot(spread.astype(BF16), v8[...].astype(BF16))
    x128 = fold(jnp.where(lane_is_t, wide, 0.0), 64, 32)

    for k in range(2):
        cond = cond_ref[k].astype(F32)
        val = val_ref[k].astype(F32)
        for v in range(4):
            at = 16 * k + 4 * v
            pairs[at : at + 4, :] = val[v : v + 1, :] * cond
    pair_rows = pairs[...].astype(BF16)
    lk[0:32, :] = pair_rows[:, :512]
    lk[32:64, :] = pair_rows[:, 512:]
    row64, lane64 = iota((64, 128), 0), iota((64, 128), 1)
    own64 = ((row64 >> 5) == ((lane64 >> 5) & 1)) & (((row64 >> 4) & 1) == (lane64 >> 6))
    x_block = jnp.where(own64, jnp.concatenate([x128, x128], axis=0), 0.0).astype(BF16)
    p_out[...] = dot(lk[...], x_block, 0, 0).astype(BF16).reshape(NR, NC, 128)

    for fetch in fetches[3:8]:
        fetch.wait()
    place = iota((1, 128), 1) - 4 * r
    k_row = jnp.zeros((1, 128), jnp.int32)
    for q in range(4):
        k_row = jnp.where(place == q, kc_ref[q // 2, q % 2], k_row)
    k_out[...] = k_row.astype(F32)

    pl.semaphore_wait(barrier, NR + NC - 2)

    def first_sends(peer):
        target = {"row": peer}
        copy_to(target, PROJ_ROW, p_out.at[peer], p_in.at[r]).start()
        copy_to(target, COORD_ROW, k_out, k_in.at[r]).start()

    peers("row", first_sends)
    k_in[pl.ds(r, 1)] = k_out[...].reshape(1, 1, 128)
    p_in[pl.ds(r, 1)] = p_out[pl.ds(r, 1)]

    for k in range(2):
        for j in range(4):
            at = 32 * j + 16 * k
            pk[at : at + 16, :] = pe_ref[k, :, j * 256 : (j + 1) * 256]
    own128 = (iota((128, 128), 0) >> 5) == (iota((128, 128), 1) >> 5)
    x_quarter = jnp.where(own128, jnp.concatenate([x128] * 4, axis=0), 0.0).astype(BF16)
    d_out[...] = dot(pk[...], x_quarter, 0, 0).reshape(NR, 8, 128)
    mine = pl.multiple_of(core * NU, NU)
    other = pl.multiple_of(NU - core * NU, NU)
    copy_to(sibling, DENS_PAIR, d_out.at[pl.ds(other, NU)], d_pair).start()

    def build_perm(i, carry):
        at = pl.multiple_of(i * 128, 128)
        row, col = iota((128, 512), 0) + i * 128, iota((128, 512), 1)
        perm_f[pl.ds(at, 128), :] = one_hot(col == ((row & 31) << 4) + (row >> 5)).astype(BF16)
        perm_b[pl.ds(at, 128), :] = one_hot(col == ((row & 15) << 5) + (row >> 4)).astype(BF16)
        return carry

    lax.fori_loop(0, 4, build_perm, 0)

    arrived_pair(DENS_PAIR, d_pair)
    d_sum[...] = d_out[pl.ds(mine, NU)] + d_pair[...]
    send("chip", DENS_ROW, lambda peer: d_sum.at[peer], d_in)
    d_in[pl.ds(chip, 1)] = d_sum[pl.ds(chip, 1)]

    energy = jnp.concatenate(
        [jnp.broadcast_to(en_ref[k : k + 1, :], (16, 16)) for k in range(2)], axis=0
    )
    same = (iota((32, 16), 0) & 15) == iota((32, 16), 1)
    e_col = jnp.sum(jnp.where(same, energy, 0.0), axis=1, keepdims=True)
    ex128 = e_col * x128
    alpha_energy = dot(x128, ex128, 0, 0, precision=HIGH)[:32]

    for fetch in fetches[8:]:
        fetch.wait()
    chosen = lax.rem(r, 8) * 16 + c
    q_row, q_lane = iota((8, 128), 0), iota((8, 128), 1)
    known = iota((QPAD, 128), 0) < NQ
    values = sum(
        dot(
            one_hot((q_row == h) & (q_lane == chosen)),
            jnp.where(known, scr[h], 0.0),
            1,
            1,
            precision=HIGH,
        )
        for h in range(2)
    )
    s_hi, s_lo = split(values)
    lam[...] = dot(s_hi, m_hi[...]) + dot(s_lo, m_hi[...]) + dot(s_hi, m_lo[...])

    arrived("row", COORD_ROW, k_in)
    h_out[...] = jnp.sum(k_in[...], axis=0)
    send("col", COORD_COL, lambda peer: h_out, h_in)
    h_in[pl.ds(c, 1)] = h_out[...].reshape(1, 1, 128)

    arrived("row", PROJ_ROW, p_in)
    mixed = dot(perm_f[...], p_in[...].reshape(512, 128)).astype(BF16)
    q_out[...] = mixed.reshape(NC, NR, 128)
    send("col", PROJ_COL, lambda peer: q_out.at[peer], q_in)
    q_in[pl.ds(c, 1)] = q_out[pl.ds(c, 1)]
    arrived("chip", DENS_ROW, d_in)
    e_out[...] = jnp.sum(d_in[...], axis=0)
    send("col", DENS_COL, lambda peer: e_out, e_in)
    e_in[pl.ds(c, 1)] = e_out[...].reshape(1, 8, 128)

    arrived("col", COORD_COL, h_in)
    for i in range(NC):
        c16[i : i + 1, :] = h_in[i]
    repeat = one_hot(iota((16, 512), 0) == (iota((16, 512), 1) >> 5)).astype(BF16)
    spread_c = dot(c16[...].astype(BF16), repeat, 0, 0)
    row128, lane512 = iota((128, 512), 0), iota((128, 512), 1)
    kept = jnp.where((row128 >> 2) == (lane512 & 31), spread_c, 0.0).astype(BF16)
    pick = one_hot((iota((128, 128), 0) >> 5) == (iota((128, 128), 1) & 3)).astype(BF16)
    coords = dot(pick, kept)
    hot = one_hot(coords == (row128 & 31).astype(F32)).astype(BF16)
    q2 = q2_ref[...]
    for k in range(2):
        at = 64 * k
        first = jnp.concatenate([hot[at : at + 32]] * 2, axis=0)
        second = jnp.concatenate([hot[at + 32 : at + 64]] * 2, axis=0)
        arow[k] = dot(q2, first)
        brow[k] = dot(q2, second)
        for i in range(4):
            at = 128 * i
            outer = dot(first[:, at : at + 128], qa_ref[...], 0, 0)
            inner = dot(second[:, at : at + 128], qb_ref[...], 0, 0)
            high, low = split(outer * inner)
            t_all[512 * k + at : 512 * k + at + 128, :] = high
            t_all[1024 + 512 * k + at : 1024 + 512 * k + at + 128, :] = low

    def build_basis(j, carry):
        at = pl.multiple_of(j * 32, 32)
        for k in range(2):
            high, low = split(arow[k, pl.ds(j, 1), :] * brow[k])
            tt_hi[k, pl.ds(at, 32), :] = high
            tt_lo[k, pl.ds(at, 32), :] = low
        return carry

    lax.fori_loop(0, 32, build_basis, 0)

    arrived("col", PROJ_COL, q_in)
    turned = jnp.transpose(q_in[...].reshape(512, 128).astype(F32)).astype(BF16)
    mode = dot(jnp.concatenate([turned[:64], turned[64:]] * 2, axis=1), t_all[...])
    first_g = iota((64, NK), 0) < 32
    scaled = jnp.where(first_g, lam[0:1, :], lam[1:2, :]) * mode
    high, low = split(scaled)
    wt[0:64, :] = high
    wt[64:128, :] = low
    for k in range(2):
        both = dot(wt[...], tt_hi[k])
        back = both[:64] + both[64:] + dot(wt[0:64, :], tt_lo[k])
        z_wide[64 * k : 64 * k + 64, :] = back
    z_out[...] = jnp.transpose(z_wide[...]).astype(BF16).reshape(NC, NR, 128)
    send("col", POT_COL, lambda peer: z_out.at[peer], z_in)
    z_in[pl.ds(c, 1)] = z_out[pl.ds(c, 1)]

    alpha_direct = dot(mode.astype(BF16), jnp.concatenate([high, high], axis=0), 1, 1)
    kept_g = jnp.where((row64 >> 5) == ((lane64 >> 5) & 1), alpha_direct, 0.0)
    part = alpha_energy - fold(kept_g[:32] + kept_g[32:], 32) * (1.0 / NK)
    a_out[...] = dot(gather8, jnp.where(lane_is_t, part, 0.0), precision=HIGH)
    send("row", ALPHA_ROW, lambda peer: a_out, a_in)
    a_in[pl.ds(r, 1)] = a_out[...].reshape(1, 8, 128)

    arrived("col", DENS_COL, e_in)
    f_out[...] = jnp.sum(e_in[...], axis=0)
    send("chip", DENS_OUT, lambda peer: f_out, f_in, base=mine)
    f_in[pl.ds(mine + chip, 1)] = f_out[...].reshape(1, 8, 128)

    c8[...] = jnp.zeros((8, 256), F32)
    for j in range(4):
        c8[j : j + 1, :] = coul_ref[:, j * 256 : (j + 1) * 256]
    expand8 = one_hot(iota((8, 128), 0) == (iota((8, 128), 1) >> 5))
    coulexp[...] = dot(c8[...], expand8, 0, 0, precision=HIGH)

    arrived("col", POT_COL, z_in)
    mixed = dot(perm_b[...], z_in[...].reshape(512, 128)).astype(BF16)
    y_out[...] = mixed.reshape(NR, NC, 128)
    send("row", POT_ROW, lambda peer: y_out.at[peer], y_in)
    y_in[pl.ds(r, 1)] = y_out[pl.ds(r, 1)]

    arrived("row", ALPHA_ROW, a_in)
    b_out[...] = jnp.sum(a_in[...], axis=0)
    send("col", ALPHA_COL, lambda peer: b_out, b_in)
    b_in[pl.ds(c, 1)] = b_out[...].reshape(1, 8, 128)

    arrived("chip", DENS_OUT, f_in)
    half = f_in.at[pl.ds(mine, NU)]
    copy_to(sibling, DENS_SWAP, half, half).start()
    arrived_pair(DENS_SWAP, f_in.at[pl.ds(other, NU)])
    density = f_in[...].reshape(256, 128)
    weighted = coulexp[...] * density
    w_hi, w_lo = split(weighted)
    quarters = pk[...]

    def total_of(v):
        v = jnp.where(own128, v, 0.0)
        return fold(v[0:32] + v[32:64] + v[64:96] + v[96:128], 64, 32)

    exchange = total_of(dot(quarters, w_hi) + dot(quarters, w_lo))
    alpha_exchange = total_of(dot(density, weighted, 0, 0, precision=HIGH))

    arrived("col", ALPHA_COL, b_in)
    shares = dot(spread, jnp.sum(b_in[...], axis=0), precision=HIGH)
    shares = fold(jnp.where(lane_is_t, shares, 0.0), 64, 32)
    alpha = (shares + (2.0 / NT) * alpha_exchange) * (1.0 / NT)
    alpha_ref[...] = alpha[:, :32]
    base = ex128 + (2.0 / NT) * exchange - dot(x128[:, :32], alpha, precision=HIGH)

    arrived("row", POT_ROW, y_in)
    direct = jnp.where(own64, dot(lk[...], y_in[...].reshape(512, 128)), 0.0)
    residual = base - fold(direct[:32] + direct[32:], 64, 32) * (1.0 / NK)
    rows = dot(gather8, jnp.where(lane_is_t, residual, 0.0), precision=HIGH)
    for i in range(8):
        out_ref[i // 4 : i // 4 + 1, (i % 4) * 128 : (i % 4 + 1) * 128] = rows[i : i + 1, :]

    for which, many in waits:
        wait_bytes(send_sems.at[which], many)


def on_device(pair_exchange, conduction, valence, coulomb, screening, energies, vectors, k_coords):
    q2, qa, qb, m_hi, m_lo = (jnp.asarray(table) for table in tables())
    operands = (
        *(pair_exchange, conduction, valence, coulomb.reshape(1, -1), energies, vectors, k_coords),
        *(q2, qa, qb, screening, m_hi, m_lo),
    )
    vmem = pl.BlockSpec(memory_space=pltpu.VMEM)
    return pl.pallas_call(
        kernel,
        out_shape=(
            jax.ShapeDtypeStruct((2, 512), F32),
            jax.ShapeDtypeStruct((32, 32), F32),
        ),
        in_specs=[pl.BlockSpec(memory_space=pltpu.HBM)] * len(operands),
        out_specs=(vmem, vmem),
        scratch_shapes=[
            pltpu.VMEM((2, 16, 1024), BF16),
            pltpu.VMEM((2, 4, 1024), BF16),
            pltpu.VMEM((2, 4, 1024), BF16),
            pltpu.VMEM((1, 1024), F32),
            pltpu.VMEM((2, 16), F32),
            pltpu.VMEM((2, 512), BF16),
            pltpu.SMEM((2, 2), jnp.int32),
            pltpu.VMEM((32, 64), BF16),
            pltpu.VMEM((64, NK), BF16),
            pltpu.VMEM((64, NK), BF16),
            pltpu.VMEM((8, 128), F32),
            pltpu.VMEM((32, 1024), F32),
            pltpu.VMEM((64, 512), BF16),
            pltpu.VMEM((128, 256), BF16),
            pltpu.VMEM((256, 128), F32),
            pltpu.VMEM((8, 256), F32),
            pltpu.VMEM((NR, NC, 128), BF16),
            pltpu.VMEM((NR, NC, 128), BF16),
            pltpu.VMEM((NC, NR, 128), BF16),
            pltpu.VMEM((NC, NR, 128), BF16),
            pltpu.VMEM((NC, NR, 128), BF16),
            pltpu.VMEM((NC, NR, 128), BF16),
            pltpu.VMEM((NR, NC, 128), BF16),
            pltpu.VMEM((NR, NC, 128), BF16),
            pltpu.VMEM((1, 128), F32),
            pltpu.VMEM((NR, 1, 128), F32),
            pltpu.VMEM((1, 128), F32),
            pltpu.VMEM((NC, 1, 128), F32),
            pltpu.VMEM((16, 128), F32),
            pltpu.VMEM((NR, 8, 128), F32),
            pltpu.VMEM((NU, 8, 128), F32),
            pltpu.VMEM((NU, 8, 128), F32),
            pltpu.VMEM((NU, 8, 128), F32),
            pltpu.VMEM((8, 128), F32),
            pltpu.VMEM((NC, 8, 128), F32),
            pltpu.VMEM((8, 128), F32),
            pltpu.VMEM((NR, 8, 128), F32),
            pltpu.VMEM((8, 128), F32),
            pltpu.VMEM((NR, 8, 128), F32),
            pltpu.VMEM((8, 128), F32),
            pltpu.VMEM((NC, 8, 128), F32),
            pltpu.VMEM((2, 32, 512), F32),
            pltpu.VMEM((2, 32, 512), F32),
            pltpu.VMEM((2048, NK), BF16),
            pltpu.VMEM((2, NK, 512), BF16),
            pltpu.VMEM((2, NK, 512), BF16),
            pltpu.VMEM((8, NK), F32),
            pltpu.VMEM((128, NK), BF16),
            pltpu.VMEM((128, 512), F32),
            pltpu.VMEM((512, 512), BF16),
            pltpu.VMEM((512, 512), BF16),
            pltpu.VMEM((2, QPAD, 128), F32),
            pltpu.VMEM((QPAD, NK), BF16),
            pltpu.VMEM((QPAD, NK), BF16),
            pltpu.SemaphoreType.DMA((13,)),
            pltpu.SemaphoreType.DMA((13,)),
            pltpu.SemaphoreType.DMA((14,)),
        ],
        compiler_params=pltpu.CompilerParams(
            collective_id=0, has_side_effects=True, vmem_limit_bytes=32 * 1024 * 1024
        ),
    )(*(pltpu.with_memory_space_constraint(v, pltpu.HBM) for v in operands))


def solution(mesh):
    split_k = ("row", "col")
    return jax.shard_map(
        on_device,
        mesh=mesh,
        in_specs=(
            P(split_k, None, None),
            P(split_k, None, None),
            P(split_k, None, None),
            P(),
            P(),
            P(split_k, None),
            P(split_k, None),
            P(split_k, None),
        ),
        out_specs=(P(split_k, None), P()),
        check_vma=False,
    )
```

```python
import jax
import jax.numpy as jnp
import numpy as np
from jax import lax
from jax.experimental import pallas as pl
from jax.experimental.pallas import tpu as pltpu
from jax.sharding import PartitionSpec as P

MESH = pl.DeviceIdType.MESH
HIGH = lax.Precision.HIGHEST
F32 = jnp.float32
BF16 = jnp.bfloat16

NR, NC, NU = 32, 16, 16
NK, NT = 1024, 16384
NQ = 289
QPAD = 384
COORD_ROW, COORD_COL, PROJ_ROW, PROJ_COL, POT_COL, POT_ROW = range(6)
DENS_PAIR, DENS_ROW, DENS_COL, DENS_OUT, DENS_SWAP = range(6, 11)
ALPHA_ROW, ALPHA_COL = range(11, 13)


def real_basis():
    points = np.arange(32)[None, :]
    order = np.arange(32)[:, None]
    freq = np.where(order <= 16, order, order - 16)
    angle = 2 * np.pi * freq * points / 32
    basis = np.where(order <= 16, np.cos(angle), np.sin(angle)) * np.sqrt(2 / 32)
    basis[[0, 16]] *= np.sqrt(0.5)
    return basis, freq[:, 0]


def two_parts(table):
    high = table.astype(BF16)
    return high, (table - high.astype(np.float64)).astype(BF16)


def tables():
    basis, freq = real_basis()
    fold = np.arange(17)
    weight = np.where((fold == 0) | (fold == 16), 1.0, 2.0)
    cosine = weight[None, :] * np.cos(2 * np.pi * freq[:, None] * fold[None, :] / 32)
    modes = np.zeros((QPAD, NK))
    modes[:NQ] = np.kron(cosine, cosine).T
    narrow = np.concatenate(two_parts(basis), axis=1)
    outer = np.concatenate(two_parts(np.repeat(basis.T, 32, axis=1)), axis=0)
    inner = np.concatenate(two_parts(np.tile(basis.T, (1, 32))), axis=0)
    return narrow, outer, inner, *two_parts(modes)


def iota(shape, dim):
    return lax.broadcasted_iota(jnp.int32, shape, dim)


def one_hot(mask):
    return jnp.where(mask, 1.0, 0.0).astype(F32)


def dot(a, b, ca=1, cb=0, precision=None):
    return lax.dot_general(
        a, b, (((ca,), (cb,)), ((), ())), precision=precision, preferred_element_type=F32
    )


def split(v):
    high = v.astype(BF16)
    return high, (v - high.astype(F32)).astype(BF16)


def fold(v, *shifts):
    for shift in shifts:
        v = v + pltpu.roll(v, shift, 1)
    return v


def kernel(
    pe_hbm, cond_hbm, val_hbm, coul_hbm, en_hbm, vec_hbm, kc_hbm, q2_hbm, qa_hbm, qb_hbm, scr_hbm,
    mhi_hbm, mlo_hbm,
    out_ref, alpha_ref,
    pe_ref, cond_ref, val_ref, coul_ref, en_ref, vec_ref, kc_ref, q2_ref, qa_ref, qb_ref,
    v8, pairs, lk, pk, coulexp, c8,
    p_out, p_in, q_out, q_in, z_out, z_in, y_out, y_in,
    k_out, k_in, h_out, h_in, c16,
    d_out, d_pair, d_sum, d_in, e_out, e_in, f_out, f_in,
    a_out, a_in, b_out, b_in,
    arow, brow, t_all, tt_hi, tt_lo, lam, wt, z_wide, perm_f, perm_b, scr, m_hi, m_lo,
    send_sems, recv_sems, local_sems,
):
    r, c = lax.axis_index("row"), lax.axis_index("col")
    core, chip = lax.rem(r, 2), r // 2
    groups = {"row": (NR, r), "col": (NC, c), "chip": (NU, chip)}

    def device(group, peer):
        if group == "chip":
            return {"row": 2 * peer + core}
        return {group: peer}

    def nth_peer(group, i):
        size, me = groups[group]
        half = size // 2
        return lax.rem(me + jnp.where(i < half, half + i, i - half + 1), size)

    def peers(group, body):
        def step(i, carry):
            body(nth_peer(group, i))
            return carry

        lax.fori_loop(0, groups[group][0] - 1, step, 0)

    def copy_to(device_id, which, source, target):
        return pltpu.make_async_remote_copy(
            src_ref=source,
            dst_ref=target,
            send_sem=send_sems.at[which],
            recv_sem=recv_sems.at[which],
            device_id=device_id,
            device_id_type=MESH,
        )

    def send(group, which, source, target, base=0):
        slot = base + groups[group][1]
        peers(
            group,
            lambda peer: copy_to(
                device(group, peer), which, source(peer), target.at[slot]
            ).start(),
        )

    def wait_bytes(sem, many):
        pltpu.make_async_copy(many, many, sem).wait()

    waits = []

    def arrived(group, which, target):
        many = target.at[pl.ds(0, groups[group][0] - 1)]
        waits.append((which, many))
        wait_bytes(recv_sems.at[which], many)

    def arrived_pair(which, target):
        waits.append((which, target))
        wait_bytes(recv_sems.at[which], target)

    sibling = {"row": r + 1 - 2 * core}

    barrier = pltpu.get_barrier_semaphore()

    def hello(i, carry):
        for axis in ("col", "row"):
            peer = nth_peer(axis, i)
            pl.semaphore_signal(barrier, inc=1, device_id={axis: peer}, device_id_type=MESH)
        return carry

    def hello_row(i, carry):
        peer = nth_peer("row", i)
        pl.semaphore_signal(barrier, inc=1, device_id={"row": peer}, device_id_type=MESH)
        return carry

    lax.fori_loop(0, NC - 1, hello, 0)
    lax.fori_loop(NC - 1, NR - 1, hello_row, 0)
    near = pl.multiple_of((r // 8) * 128, 128)
    far = pl.multiple_of((r // 8) * 128 + 512, 128)
    fetches = [
        pltpu.make_async_copy(source, target, local_sems.at[i])
        for i, (source, target) in enumerate(
            (
                (vec_hbm, vec_ref),
                (cond_hbm, cond_ref),
                (val_hbm, val_ref),
                (kc_hbm, kc_ref),
                (pe_hbm, pe_ref),
                (coul_hbm, coul_ref),
                (en_hbm, en_ref),
                (q2_hbm, q2_ref),
                (scr_hbm.at[:, pl.ds(near, 128)], scr.at[0, pl.ds(0, NQ), :]),
                (scr_hbm.at[:, pl.ds(far, 128)], scr.at[1, pl.ds(0, NQ), :]),
                (mhi_hbm, m_hi),
                (mlo_hbm, m_lo),
                (qa_hbm, qa_ref),
                (qb_hbm, qb_ref),
            )
        )
    ]
    for fetch in fetches:
        fetch.start()
    for fetch in fetches[:3]:
        fetch.wait()

    vec = vec_ref[...].astype(F32)
    for i in range(8):
        v8[i : i + 1, :] = vec[i // 4 : i // 4 + 1, (i % 4) * 128 : (i % 4 + 1) * 128]
    row32, lane32 = iota((32, 128), 0), iota((32, 128), 1)
    lane_is_t = (row32 & 3) == (lane32 >> 5)
    spread = one_hot((iota((32, 8), 0) >> 2) == iota((32, 8), 1))
    gather8 = one_hot((iota((8, 32), 1) >> 2) == iota((8, 32), 0))
    wide = dot(spread.astype(BF16), v8[...].astype(BF16))
    x128 = fold(jnp.where(lane_is_t, wide, 0.0), 64, 32)

    for k in range(2):
        cond = cond_ref[k].astype(F32)
        val = val_ref[k].astype(F32)
        for v in range(4):
            at = 16 * k + 4 * v
            pairs[at : at + 4, :] = val[v : v + 1, :] * cond
    pair_rows = pairs[...].astype(BF16)
    lk[0:32, :] = pair_rows[:, :512]
    lk[32:64, :] = pair_rows[:, 512:]
    row64, lane64 = iota((64, 128), 0), iota((64, 128), 1)
    own64 = ((row64 >> 5) == ((lane64 >> 5) & 1)) & (((row64 >> 4) & 1) == (lane64 >> 6))
    x_block = jnp.where(own64, jnp.concatenate([x128, x128], axis=0), 0.0).astype(BF16)
    p_out[...] = dot(lk[...], x_block, 0, 0).astype(BF16).reshape(NR, NC, 128)

    for fetch in fetches[3:8]:
        fetch.wait()
    place = iota((1, 128), 1) - 4 * r
    k_row = jnp.zeros((1, 128), jnp.int32)
    for q in range(4):
        k_row = jnp.where(place == q, kc_ref[q // 2, q % 2], k_row)
    k_out[...] = k_row.astype(F32)

    pl.semaphore_wait(barrier, NR + NC - 2)
    send("row", COORD_ROW, lambda peer: k_out, k_in)
    send("row", PROJ_ROW, lambda peer: p_out.at[peer], p_in)
    k_in[pl.ds(r, 1)] = k_out[...].reshape(1, 1, 128)
    p_in[pl.ds(r, 1)] = p_out[pl.ds(r, 1)]

    for k in range(2):
        for j in range(4):
            at = 32 * j + 16 * k
            pk[at : at + 16, :] = pe_ref[k, :, j * 256 : (j + 1) * 256]
    own128 = (iota((128, 128), 0) >> 5) == (iota((128, 128), 1) >> 5)
    x_quarter = jnp.where(own128, jnp.concatenate([x128] * 4, axis=0), 0.0).astype(BF16)
    d_out[...] = dot(pk[...], x_quarter, 0, 0).reshape(NR, 8, 128)
    mine = pl.multiple_of(core * NU, NU)
    other = pl.multiple_of(NU - core * NU, NU)
    copy_to(sibling, DENS_PAIR, d_out.at[pl.ds(other, NU)], d_pair).start()

    def build_perm(i, carry):
        at = pl.multiple_of(i * 128, 128)
        row, col = iota((128, 512), 0) + i * 128, iota((128, 512), 1)
        perm_f[pl.ds(at, 128), :] = one_hot(col == ((row & 31) << 4) + (row >> 5)).astype(BF16)
        perm_b[pl.ds(at, 128), :] = one_hot(col == ((row & 15) << 5) + (row >> 4)).astype(BF16)
        return carry

    lax.fori_loop(0, 4, build_perm, 0)

    arrived_pair(DENS_PAIR, d_pair)
    d_sum[...] = d_out[pl.ds(mine, NU)] + d_pair[...]
    send("chip", DENS_ROW, lambda peer: d_sum.at[peer], d_in)
    d_in[pl.ds(chip, 1)] = d_sum[pl.ds(chip, 1)]

    energy = jnp.concatenate(
        [jnp.broadcast_to(en_ref[k : k + 1, :], (16, 16)) for k in range(2)], axis=0
    )
    same = (iota((32, 16), 0) & 15) == iota((32, 16), 1)
    e_col = jnp.sum(jnp.where(same, energy, 0.0), axis=1, keepdims=True)
    ex128 = e_col * x128
    alpha_energy = dot(x128, ex128, 0, 0, precision=HIGH)[:32]

    for fetch in fetches[8:]:
        fetch.wait()
    chosen = lax.rem(r, 8) * 16 + c
    q_row, q_lane = iota((8, 128), 0), iota((8, 128), 1)
    known = iota((QPAD, 128), 0) < NQ
    values = sum(
        dot(
            one_hot((q_row == h) & (q_lane == chosen)),
            jnp.where(known, scr[h], 0.0),
            1,
            1,
            precision=HIGH,
        )
        for h in range(2)
    )
    s_hi, s_lo = split(values)
    lam[...] = dot(s_hi, m_hi[...]) + dot(s_lo, m_hi[...]) + dot(s_hi, m_lo[...])

    arrived("row", COORD_ROW, k_in)
    h_out[...] = jnp.sum(k_in[...], axis=0)
    send("col", COORD_COL, lambda peer: h_out, h_in)
    h_in[pl.ds(c, 1)] = h_out[...].reshape(1, 1, 128)

    arrived("row", PROJ_ROW, p_in)
    mixed = dot(perm_f[...], p_in[...].reshape(512, 128)).astype(BF16)
    q_out[...] = mixed.reshape(NC, NR, 128)
    send("col", PROJ_COL, lambda peer: q_out.at[peer], q_in)
    q_in[pl.ds(c, 1)] = q_out[pl.ds(c, 1)]
    arrived("chip", DENS_ROW, d_in)
    e_out[...] = jnp.sum(d_in[...], axis=0)
    send("col", DENS_COL, lambda peer: e_out, e_in)
    e_in[pl.ds(c, 1)] = e_out[...].reshape(1, 8, 128)

    arrived("col", COORD_COL, h_in)
    for i in range(NC):
        c16[i : i + 1, :] = h_in[i]
    repeat = one_hot(iota((16, 512), 0) == (iota((16, 512), 1) >> 5)).astype(BF16)
    spread_c = dot(c16[...].astype(BF16), repeat, 0, 0)
    row128, lane512 = iota((128, 512), 0), iota((128, 512), 1)
    kept = jnp.where((row128 >> 2) == (lane512 & 31), spread_c, 0.0).astype(BF16)
    pick = one_hot((iota((128, 128), 0) >> 5) == (iota((128, 128), 1) & 3)).astype(BF16)
    coords = dot(pick, kept)
    hot = one_hot(coords == (row128 & 31).astype(F32)).astype(BF16)
    q2 = q2_ref[...]
    for k in range(2):
        at = 64 * k
        first = jnp.concatenate([hot[at : at + 32]] * 2, axis=0)
        second = jnp.concatenate([hot[at + 32 : at + 64]] * 2, axis=0)
        arow[k] = dot(q2, first)
        brow[k] = dot(q2, second)
        for i in range(4):
            at = 128 * i
            outer = dot(first[:, at : at + 128], qa_ref[...], 0, 0)
            inner = dot(second[:, at : at + 128], qb_ref[...], 0, 0)
            high, low = split(outer * inner)
            t_all[512 * k + at : 512 * k + at + 128, :] = high
            t_all[1024 + 512 * k + at : 1024 + 512 * k + at + 128, :] = low

    def build_basis(j, carry):
        at = pl.multiple_of(j * 32, 32)
        for k in range(2):
            high, low = split(arow[k, pl.ds(j, 1), :] * brow[k])
            tt_hi[k, pl.ds(at, 32), :] = high
            tt_lo[k, pl.ds(at, 32), :] = low
        return carry

    lax.fori_loop(0, 32, build_basis, 0)

    arrived("col", PROJ_COL, q_in)
    turned = jnp.transpose(q_in[...].reshape(512, 128).astype(F32)).astype(BF16)
    mode = dot(jnp.concatenate([turned[:64], turned[64:]] * 2, axis=1), t_all[...])
    first_g = iota((64, NK), 0) < 32
    scaled = jnp.where(first_g, lam[0:1, :], lam[1:2, :]) * mode
    high, low = split(scaled)
    wt[0:64, :] = high
    wt[64:128, :] = low
    for k in range(2):
        both = dot(wt[...], tt_hi[k])
        back = both[:64] + both[64:] + dot(wt[0:64, :], tt_lo[k])
        z_wide[64 * k : 64 * k + 64, :] = back
    z_out[...] = jnp.transpose(z_wide[...]).astype(BF16).reshape(NC, NR, 128)
    send("col", POT_COL, lambda peer: z_out.at[peer], z_in)
    z_in[pl.ds(c, 1)] = z_out[pl.ds(c, 1)]

    alpha_direct = dot(mode.astype(BF16), jnp.concatenate([high, high], axis=0), 1, 1)
    kept_g = jnp.where((row64 >> 5) == ((lane64 >> 5) & 1), alpha_direct, 0.0)
    part = alpha_energy - fold(kept_g[:32] + kept_g[32:], 32) * (1.0 / NK)
    packed = dot(gather8, jnp.where(lane_is_t, part, 0.0), precision=HIGH)
    a_out[...] = packed.astype(BF16)
    send("row", ALPHA_ROW, lambda peer: a_out, a_in)
    a_in[pl.ds(r, 1)] = a_out[...].reshape(1, 8, 128)

    arrived("col", DENS_COL, e_in)
    f_out[...] = jnp.sum(e_in[...], axis=0)
    send("chip", DENS_OUT, lambda peer: f_out, f_in, base=mine)
    f_in[pl.ds(mine + chip, 1)] = f_out[...].reshape(1, 8, 128)

    c8[...] = jnp.zeros((8, 256), F32)
    for j in range(4):
        c8[j : j + 1, :] = coul_ref[:, j * 256 : (j + 1) * 256]
    expand8 = one_hot(iota((8, 128), 0) == (iota((8, 128), 1) >> 5))
    coulexp[...] = dot(c8[...], expand8, 0, 0, precision=HIGH)

    arrived("col", POT_COL, z_in)
    mixed = dot(perm_b[...], z_in[...].reshape(512, 128)).astype(BF16)
    y_out[...] = mixed.reshape(NR, NC, 128)
    send("row", POT_ROW, lambda peer: y_out.at[peer], y_in)
    y_in[pl.ds(r, 1)] = y_out[pl.ds(r, 1)]

    arrived("row", ALPHA_ROW, a_in)
    b_out[...] = jnp.sum(a_in[...].astype(F32), axis=0)
    send("col", ALPHA_COL, lambda peer: b_out, b_in)
    b_in[pl.ds(c, 1)] = b_out[...].reshape(1, 8, 128)

    arrived("chip", DENS_OUT, f_in)
    half = f_in.at[pl.ds(mine, NU)]
    copy_to(sibling, DENS_SWAP, half, half).start()
    arrived_pair(DENS_SWAP, f_in.at[pl.ds(other, NU)])
    density = f_in[...].reshape(256, 128)
    weighted = coulexp[...] * density
    w_hi, w_lo = split(weighted)
    quarters = pk[...]

    def total_of(v):
        v = jnp.where(own128, v, 0.0)
        return fold(v[0:32] + v[32:64] + v[64:96] + v[96:128], 64, 32)

    exchange = total_of(dot(quarters, w_hi) + dot(quarters, w_lo))
    alpha_exchange = total_of(dot(density, weighted, 0, 0, precision=HIGH)) * (2.0 / NT / NT)
    x32 = x128[:, :32]
    base = ex128 + (2.0 / NT) * exchange - dot(x32, alpha_exchange, precision=HIGH)
    base = jnp.where(lane_is_t, base, 0.0)
    pick_m = iota((32, 8), 0)
    x_by_u = jnp.concatenate(
        [dot(x32, one_hot(pick_m == 4 * iota((32, 8), 1) + u), precision=HIGH) for u in range(4)],
        axis=0,
    )

    def four_blocks(v):
        v = jnp.where(own128, v, 0.0)
        return v[0:32] + v[32:64] + v[64:96] + v[96:128]

    arrived("col", ALPHA_COL, b_in)
    shares = jnp.sum(b_in[...], axis=0) * (1.0 / NT)
    projected = four_blocks(dot(x_by_u, shares, precision=HIGH))

    arrived("row", POT_ROW, y_in)
    direct = jnp.where(own64, dot(lk[...], y_in[...].reshape(512, 128)), 0.0)
    both = fold(projected + (direct[:32] + direct[32:]) * (1.0 / NK), 64, 32)
    rows = base - jnp.where(lane_is_t, both, 0.0)
    rows = rows + pltpu.roll(rows, 31, 0)
    rows = rows + pltpu.roll(rows, 30, 0)
    for i in range(8):
        at = 128 * (i % 4)
        out_ref[i // 4 : i // 4 + 1, at : at + 128] = rows[4 * i : 4 * i + 1, :]
    alpha = fold(jnp.where(lane_is_t, dot(spread, shares, precision=HIGH), 0.0), 64, 32)
    alpha_ref[...] = (alpha + alpha_exchange)[:, :32]

    for which, many in waits:
        wait_bytes(send_sems.at[which], many)


def on_device(pair_exchange, conduction, valence, coulomb, screening, energies, vectors, k_coords):
    q2, qa, qb, m_hi, m_lo = (jnp.asarray(table) for table in tables())
    operands = (
        *(pair_exchange, conduction, valence, coulomb.reshape(1, -1), energies, vectors, k_coords),
        *(q2, qa, qb, screening, m_hi, m_lo),
    )
    vmem = pl.BlockSpec(memory_space=pltpu.VMEM)
    return pl.pallas_call(
        kernel,
        out_shape=(
            jax.ShapeDtypeStruct((2, 512), F32),
            jax.ShapeDtypeStruct((32, 32), F32),
        ),
        in_specs=[pl.BlockSpec(memory_space=pltpu.HBM)] * len(operands),
        out_specs=(vmem, vmem),
        scratch_shapes=[
            pltpu.VMEM((2, 16, 1024), BF16),
            pltpu.VMEM((2, 4, 1024), BF16),
            pltpu.VMEM((2, 4, 1024), BF16),
            pltpu.VMEM((1, 1024), F32),
            pltpu.VMEM((2, 16), F32),
            pltpu.VMEM((2, 512), BF16),
            pltpu.SMEM((2, 2), jnp.int32),
            pltpu.VMEM((32, 64), BF16),
            pltpu.VMEM((64, NK), BF16),
            pltpu.VMEM((64, NK), BF16),
            pltpu.VMEM((8, 128), F32),
            pltpu.VMEM((32, 1024), F32),
            pltpu.VMEM((64, 512), BF16),
            pltpu.VMEM((128, 256), BF16),
            pltpu.VMEM((256, 128), F32),
            pltpu.VMEM((8, 256), F32),
            pltpu.VMEM((NR, NC, 128), BF16),
            pltpu.VMEM((NR, NC, 128), BF16),
            pltpu.VMEM((NC, NR, 128), BF16),
            pltpu.VMEM((NC, NR, 128), BF16),
            pltpu.VMEM((NC, NR, 128), BF16),
            pltpu.VMEM((NC, NR, 128), BF16),
            pltpu.VMEM((NR, NC, 128), BF16),
            pltpu.VMEM((NR, NC, 128), BF16),
            pltpu.VMEM((1, 128), F32),
            pltpu.VMEM((NR, 1, 128), F32),
            pltpu.VMEM((1, 128), F32),
            pltpu.VMEM((NC, 1, 128), F32),
            pltpu.VMEM((16, 128), F32),
            pltpu.VMEM((NR, 8, 128), F32),
            pltpu.VMEM((NU, 8, 128), F32),
            pltpu.VMEM((NU, 8, 128), F32),
            pltpu.VMEM((NU, 8, 128), F32),
            pltpu.VMEM((8, 128), F32),
            pltpu.VMEM((NC, 8, 128), F32),
            pltpu.VMEM((8, 128), F32),
            pltpu.VMEM((NR, 8, 128), F32),
            pltpu.VMEM((8, 128), BF16),
            pltpu.VMEM((NR, 8, 128), BF16),
            pltpu.VMEM((8, 128), F32),
            pltpu.VMEM((NC, 8, 128), F32),
            pltpu.VMEM((2, 32, 512), F32),
            pltpu.VMEM((2, 32, 512), F32),
            pltpu.VMEM((2048, NK), BF16),
            pltpu.VMEM((2, NK, 512), BF16),
            pltpu.VMEM((2, NK, 512), BF16),
            pltpu.VMEM((8, NK), F32),
            pltpu.VMEM((128, NK), BF16),
            pltpu.VMEM((128, 512), F32),
            pltpu.VMEM((512, 512), BF16),
            pltpu.VMEM((512, 512), BF16),
            pltpu.VMEM((2, QPAD, 128), F32),
            pltpu.VMEM((QPAD, NK), BF16),
            pltpu.VMEM((QPAD, NK), BF16),
            pltpu.SemaphoreType.DMA((13,)),
            pltpu.SemaphoreType.DMA((13,)),
            pltpu.SemaphoreType.DMA((14,)),
        ],
        compiler_params=pltpu.CompilerParams(
            collective_id=0, has_side_effects=True, vmem_limit_bytes=32 * 1024 * 1024
        ),
    )(*(pltpu.with_memory_space_constraint(v, pltpu.HBM) for v in operands))


def solution(mesh):
    split_k = ("row", "col")
    return jax.shard_map(
        on_device,
        mesh=mesh,
        in_specs=(
            P(split_k, None, None),
            P(split_k, None, None),
            P(split_k, None, None),
            P(),
            P(),
            P(split_k, None),
            P(split_k, None),
            P(split_k, None),
        ),
        out_specs=(P(split_k, None), P()),
        check_vma=False,
    )
```

```python
import jax
import jax.numpy as jnp
import numpy as np
from jax import lax
from jax.experimental import pallas as pl
from jax.experimental.pallas import tpu as pltpu
from jax.sharding import PartitionSpec as P

MESH = pl.DeviceIdType.MESH
HIGH = lax.Precision.HIGHEST
F32 = jnp.float32
BF16 = jnp.bfloat16

NR, NC, NU = 32, 16, 16
NK, NT = 1024, 16384
NQ = 289
QPAD = 384
COORD_ROW, COORD_COL, PROJ_ROW, PROJ_COL, POT_COL, POT_ROW = range(6)
DENS_PAIR, DENS_ROW, DENS_COL, DENS_OUT, DENS_SWAP = range(6, 11)
ALPHA_ROW, ALPHA_COL = range(11, 13)


def real_basis():
    points = np.arange(32)[None, :]
    order = np.arange(32)[:, None]
    freq = np.where(order <= 16, order, order - 16)
    angle = 2 * np.pi * freq * points / 32
    basis = np.where(order <= 16, np.cos(angle), np.sin(angle)) * np.sqrt(2 / 32)
    basis[[0, 16]] *= np.sqrt(0.5)
    return basis, freq[:, 0]


def two_parts(table):
    high = table.astype(BF16)
    return high, (table - high.astype(np.float64)).astype(BF16)


def tables():
    basis, freq = real_basis()
    fold = np.arange(17)
    weight = np.where((fold == 0) | (fold == 16), 1.0, 2.0)
    cosine = weight[None, :] * np.cos(2 * np.pi * freq[:, None] * fold[None, :] / 32)
    modes = np.zeros((QPAD, NK))
    modes[:NQ] = np.kron(cosine, cosine).T
    narrow = np.concatenate(two_parts(basis), axis=1)
    outer = np.concatenate(two_parts(np.repeat(basis.T, 32, axis=1)), axis=0)
    inner = np.concatenate(two_parts(np.tile(basis.T, (1, 32))), axis=0)
    return narrow, outer, inner, *two_parts(modes)


def iota(shape, dim):
    return lax.broadcasted_iota(jnp.int32, shape, dim)


def one_hot(mask):
    return jnp.where(mask, 1.0, 0.0).astype(F32)


def dot(a, b, ca=1, cb=0, precision=None):
    return lax.dot_general(
        a, b, (((ca,), (cb,)), ((), ())), precision=precision, preferred_element_type=F32
    )


def split(v):
    high = v.astype(BF16)
    return high, (v - high.astype(F32)).astype(BF16)


def fold(v, *shifts):
    for shift in shifts:
        v = v + pltpu.roll(v, shift, 1)
    return v


def kernel(
    pe_hbm, cond_hbm, val_hbm, coul_hbm, en_hbm, vec_hbm, kc_hbm, q2_hbm, qa_hbm, qb_hbm, scr_hbm,
    mhi_hbm, mlo_hbm,
    out_ref, alpha_ref,
    pe_ref, cond_ref, val_ref, coul_ref, en_ref, vec_ref, kc_ref, q2_ref, qa_ref, qb_ref,
    v8, pairs, lk, pk, coulexp, c8,
    p_out, p_in, q_out, q_in, z_out, z_in, y_out, y_in,
    k_out, k_in, h_out, h_in, c16,
    d_out, d_pair, d_sum, d_in, e_out, e_in, f_out, f_in,
    a_out, a_in, b_out, b_in,
    arow, brow, t_all, tt_hi, tt_lo, lam, wt, z_wide, perm_f, perm_b, scr, m_hi, m_lo,
    send_sems, recv_sems, local_sems,
):
    r, c = lax.axis_index("row"), lax.axis_index("col")
    core, chip = lax.rem(r, 2), r // 2
    groups = {"row": (NR, r), "col": (NC, c), "chip": (NU, chip)}

    def device(group, peer):
        if group == "chip":
            return {"row": 2 * peer + core}
        return {group: peer}

    def nth_peer(group, i):
        me = groups[group][1]
        if group == "col":
            ways = jnp.where(lax.rem(i, 2) == 0, 1, 3)
            y_step = jnp.where(i < 4, 2, jnp.where(i >= 12, 0, ways))
            at = jnp.where((i >= 4) & (i < 12), (i - 4) // 2, lax.rem(i, 4))
            x_step = jnp.where(at == 3, 0, jnp.where(at == 2, 3, 2 - at))
            return lax.rem(me // 4 + x_step, 4) * 4 + lax.rem(lax.rem(me, 4) + y_step, 4)
        inner = groups[group][0] // 8
        at = i // inner
        z_step = jnp.where(lax.rem(at, 2) == 1, 4 - (at + 1) // 2, 4 + at // 2)
        z_step = jnp.where(at == 7, 0, z_step)
        near = lax.rem(lax.rem(me, inner) + lax.rem(i, inner) + 1, inner)
        return lax.rem(me // inner + z_step, 8) * inner + near

    def peers(group, body):
        def step(i, carry):
            body(nth_peer(group, i))
            return carry

        lax.fori_loop(0, groups[group][0] - 1, step, 0)

    def copy_to(device_id, which, source, target):
        return pltpu.make_async_remote_copy(
            src_ref=source,
            dst_ref=target,
            send_sem=send_sems.at[which],
            recv_sem=recv_sems.at[which],
            device_id=device_id,
            device_id_type=MESH,
        )

    def send(group, which, source, target, base=0):
        slot = base + groups[group][1]
        peers(
            group,
            lambda peer: copy_to(
                device(group, peer), which, source(peer), target.at[slot]
            ).start(),
        )

    def wait_bytes(sem, many):
        pltpu.make_async_copy(many, many, sem).wait()

    waits = []

    def arrived(group, which, target):
        many = target.at[pl.ds(0, groups[group][0] - 1)]
        waits.append((which, many))
        wait_bytes(recv_sems.at[which], many)

    def arrived_pair(which, target):
        waits.append((which, target))
        wait_bytes(recv_sems.at[which], target)

    sibling = {"row": r + 1 - 2 * core}

    barrier = pltpu.get_barrier_semaphore()

    def hello(i, carry):
        for axis in ("col", "row"):
            peer = nth_peer(axis, i)
            pl.semaphore_signal(barrier, inc=1, device_id={axis: peer}, device_id_type=MESH)
        return carry

    def hello_row(i, carry):
        peer = nth_peer("row", i)
        pl.semaphore_signal(barrier, inc=1, device_id={"row": peer}, device_id_type=MESH)
        return carry

    lax.fori_loop(0, NC - 1, hello, 0)
    lax.fori_loop(NC - 1, NR - 1, hello_row, 0)
    near = pl.multiple_of((r // 8) * 128, 128)
    far = pl.multiple_of((r // 8) * 128 + 512, 128)
    fetches = [
        pltpu.make_async_copy(source, target, local_sems.at[i])
        for i, (source, target) in enumerate(
            (
                (vec_hbm, vec_ref),
                (cond_hbm, cond_ref),
                (val_hbm, val_ref),
                (kc_hbm, kc_ref),
                (pe_hbm, pe_ref),
                (coul_hbm, coul_ref),
                (en_hbm, en_ref),
                (q2_hbm, q2_ref),
                (scr_hbm.at[:, pl.ds(near, 128)], scr.at[0, pl.ds(0, NQ), :]),
                (scr_hbm.at[:, pl.ds(far, 128)], scr.at[1, pl.ds(0, NQ), :]),
                (mhi_hbm, m_hi),
                (mlo_hbm, m_lo),
                (qa_hbm, qa_ref),
                (qb_hbm, qb_ref),
            )
        )
    ]
    for fetch in fetches:
        fetch.start()
    for fetch in fetches[:3]:
        fetch.wait()

    vec = vec_ref[...].astype(F32)
    for i in range(8):
        v8[i : i + 1, :] = vec[i // 4 : i // 4 + 1, (i % 4) * 128 : (i % 4 + 1) * 128]
    row32, lane32 = iota((32, 128), 0), iota((32, 128), 1)
    lane_is_t = (row32 & 3) == (lane32 >> 5)
    spread = one_hot((iota((32, 8), 0) >> 2) == iota((32, 8), 1))
    gather8 = one_hot((iota((8, 32), 1) >> 2) == iota((8, 32), 0))
    wide = dot(spread.astype(BF16), v8[...].astype(BF16))
    x128 = fold(jnp.where(lane_is_t, wide, 0.0), 64, 32)

    for k in range(2):
        cond = cond_ref[k].astype(F32)
        val = val_ref[k].astype(F32)
        for v in range(4):
            at = 16 * k + 4 * v
            pairs[at : at + 4, :] = val[v : v + 1, :] * cond
    pair_rows = pairs[...].astype(BF16)
    lk[0:32, :] = pair_rows[:, :512]
    lk[32:64, :] = pair_rows[:, 512:]
    row64, lane64 = iota((64, 128), 0), iota((64, 128), 1)
    own64 = ((row64 >> 5) == ((lane64 >> 5) & 1)) & (((row64 >> 4) & 1) == (lane64 >> 6))
    x_block = jnp.where(own64, jnp.concatenate([x128, x128], axis=0), 0.0).astype(BF16)
    p_out[...] = dot(lk[...], x_block, 0, 0).astype(BF16).reshape(NR, NC, 128)

    for fetch in fetches[3:8]:
        fetch.wait()
    place = iota((1, 128), 1) - 4 * r
    k_row = jnp.zeros((1, 128), jnp.int32)
    for q in range(4):
        k_row = jnp.where(place == q, kc_ref[q // 2, q % 2], k_row)
    k_out[...] = k_row.astype(F32)

    pl.semaphore_wait(barrier, NR + NC - 2)
    send("row", COORD_ROW, lambda peer: k_out, k_in)
    send("row", PROJ_ROW, lambda peer: p_out.at[peer], p_in)
    k_in[pl.ds(r, 1)] = k_out[...].reshape(1, 1, 128)
    p_in[pl.ds(r, 1)] = p_out[pl.ds(r, 1)]

    for k in range(2):
        for j in range(4):
            at = 32 * j + 16 * k
            pk[at : at + 16, :] = pe_ref[k, :, j * 256 : (j + 1) * 256]
    own128 = (iota((128, 128), 0) >> 5) == (iota((128, 128), 1) >> 5)
    x_quarter = jnp.where(own128, jnp.concatenate([x128] * 4, axis=0), 0.0).astype(BF16)
    d_out[...] = dot(pk[...], x_quarter, 0, 0).reshape(NR, 8, 128)
    mine = pl.multiple_of(core * NU, NU)
    other = pl.multiple_of(NU - core * NU, NU)
    copy_to(sibling, DENS_PAIR, d_out.at[pl.ds(other, NU)], d_pair).start()

    def build_perm(i, carry):
        at = pl.multiple_of(i * 128, 128)
        row, col = iota((128, 512), 0) + i * 128, iota((128, 512), 1)
        perm_f[pl.ds(at, 128), :] = one_hot(col == ((row & 31) << 4) + (row >> 5)).astype(BF16)
        perm_b[pl.ds(at, 128), :] = one_hot(col == ((row & 15) << 5) + (row >> 4)).astype(BF16)
        return carry

    lax.fori_loop(0, 4, build_perm, 0)

    arrived_pair(DENS_PAIR, d_pair)
    d_sum[...] = d_out[pl.ds(mine, NU)] + d_pair[...]
    send("chip", DENS_ROW, lambda peer: d_sum.at[peer], d_in)
    d_in[pl.ds(chip, 1)] = d_sum[pl.ds(chip, 1)]

    energy = jnp.concatenate(
        [jnp.broadcast_to(en_ref[k : k + 1, :], (16, 16)) for k in range(2)], axis=0
    )
    same = (iota((32, 16), 0) & 15) == iota((32, 16), 1)
    e_col = jnp.sum(jnp.where(same, energy, 0.0), axis=1, keepdims=True)
    ex128 = e_col * x128
    alpha_energy = dot(x128, ex128, 0, 0, precision=HIGH)[:32]

    for fetch in fetches[8:]:
        fetch.wait()
    chosen = lax.rem(r, 8) * 16 + c
    q_row, q_lane = iota((8, 128), 0), iota((8, 128), 1)
    known = iota((QPAD, 128), 0) < NQ
    values = sum(
        dot(
            one_hot((q_row == h) & (q_lane == chosen)),
            jnp.where(known, scr[h], 0.0),
            1,
            1,
            precision=HIGH,
        )
        for h in range(2)
    )
    s_hi, s_lo = split(values)
    lam[...] = dot(s_hi, m_hi[...]) + dot(s_lo, m_hi[...]) + dot(s_hi, m_lo[...])

    arrived("row", COORD_ROW, k_in)
    h_out[...] = jnp.sum(k_in[...], axis=0)
    send("col", COORD_COL, lambda peer: h_out, h_in)
    h_in[pl.ds(c, 1)] = h_out[...].reshape(1, 1, 128)

    arrived("row", PROJ_ROW, p_in)
    mixed = dot(perm_f[...], p_in[...].reshape(512, 128)).astype(BF16)
    q_out[...] = mixed.reshape(NC, NR, 128)
    send("col", PROJ_COL, lambda peer: q_out.at[peer], q_in)
    q_in[pl.ds(c, 1)] = q_out[pl.ds(c, 1)]
    arrived("chip", DENS_ROW, d_in)
    e_out[...] = jnp.sum(d_in[...], axis=0)
    send("col", DENS_COL, lambda peer: e_out, e_in)
    e_in[pl.ds(c, 1)] = e_out[...].reshape(1, 8, 128)

    arrived("col", COORD_COL, h_in)
    for i in range(NC):
        c16[i : i + 1, :] = h_in[i]
    repeat = one_hot(iota((16, 512), 0) == (iota((16, 512), 1) >> 5)).astype(BF16)
    spread_c = dot(c16[...].astype(BF16), repeat, 0, 0)
    row128, lane512 = iota((128, 512), 0), iota((128, 512), 1)
    kept = jnp.where((row128 >> 2) == (lane512 & 31), spread_c, 0.0).astype(BF16)
    pick = one_hot((iota((128, 128), 0) >> 5) == (iota((128, 128), 1) & 3)).astype(BF16)
    coords = dot(pick, kept)
    hot = one_hot(coords == (row128 & 31).astype(F32)).astype(BF16)
    q2 = q2_ref[...]
    for k in range(2):
        at = 64 * k
        first = jnp.concatenate([hot[at : at + 32]] * 2, axis=0)
        second = jnp.concatenate([hot[at + 32 : at + 64]] * 2, axis=0)
        arow[k] = dot(q2, first)
        brow[k] = dot(q2, second)
        for i in range(4):
            at = 128 * i
            outer = dot(first[:, at : at + 128], qa_ref[...], 0, 0)
            inner = dot(second[:, at : at + 128], qb_ref[...], 0, 0)
            high, low = split(outer * inner)
            t_all[512 * k + at : 512 * k + at + 128, :] = high
            t_all[1024 + 512 * k + at : 1024 + 512 * k + at + 128, :] = low

    def build_basis(j, carry):
        at = pl.multiple_of(j * 32, 32)
        for k in range(2):
            high, low = split(arow[k, pl.ds(j, 1), :] * brow[k])
            tt_hi[k, pl.ds(at, 32), :] = high
            tt_lo[k, pl.ds(at, 32), :] = low
        return carry

    lax.fori_loop(0, 32, build_basis, 0)

    arrived("col", PROJ_COL, q_in)
    turned = jnp.transpose(q_in[...].reshape(512, 128).astype(F32)).astype(BF16)
    mode = dot(jnp.concatenate([turned[:64], turned[64:]] * 2, axis=1), t_all[...])
    first_g = iota((64, NK), 0) < 32
    scaled = jnp.where(first_g, lam[0:1, :], lam[1:2, :]) * mode
    high, low = split(scaled)
    wt[0:64, :] = high
    wt[64:128, :] = low
    alpha_direct = dot(mode.astype(BF16), jnp.concatenate([high, high], axis=0), 1, 1)
    kept_g = jnp.where((row64 >> 5) == ((lane64 >> 5) & 1), alpha_direct, 0.0)
    part = alpha_energy - fold(kept_g[:32] + kept_g[32:], 32) * (1.0 / NK)
    packed = dot(gather8, jnp.where(lane_is_t, part, 0.0), precision=HIGH)
    a_out[...] = packed.astype(BF16)

    for k in range(2):
        both = dot(wt[...], tt_hi[k])
        back = both[:64] + both[64:] + dot(wt[0:64, :], tt_lo[k])
        z_wide[64 * k : 64 * k + 64, :] = back
    z_out[...] = jnp.transpose(z_wide[...]).astype(BF16).reshape(NC, NR, 128)
    send("col", POT_COL, lambda peer: z_out.at[peer], z_in)
    z_in[pl.ds(c, 1)] = z_out[pl.ds(c, 1)]

    send("row", ALPHA_ROW, lambda peer: a_out, a_in)
    a_in[pl.ds(r, 1)] = a_out[...].reshape(1, 8, 128)

    arrived("col", DENS_COL, e_in)
    f_out[...] = jnp.sum(e_in[...], axis=0)
    send("chip", DENS_OUT, lambda peer: f_out, f_in, base=mine)
    f_in[pl.ds(mine + chip, 1)] = f_out[...].reshape(1, 8, 128)

    c8[...] = jnp.zeros((8, 256), F32)
    for j in range(4):
        c8[j : j + 1, :] = coul_ref[:, j * 256 : (j + 1) * 256]
    expand8 = one_hot(iota((8, 128), 0) == (iota((8, 128), 1) >> 5))
    coulexp[...] = dot(c8[...], expand8, 0, 0, precision=HIGH)

    arrived("col", POT_COL, z_in)
    mixed = dot(perm_b[...], z_in[...].reshape(512, 128)).astype(BF16)
    y_out[...] = mixed.reshape(NR, NC, 128)
    send("row", POT_ROW, lambda peer: y_out.at[peer], y_in)
    y_in[pl.ds(r, 1)] = y_out[pl.ds(r, 1)]

    arrived("row", ALPHA_ROW, a_in)
    b_out[...] = jnp.sum(a_in[...].astype(F32), axis=0)
    send("col", ALPHA_COL, lambda peer: b_out, b_in)
    b_in[pl.ds(c, 1)] = b_out[...].reshape(1, 8, 128)

    arrived("chip", DENS_OUT, f_in)
    half = f_in.at[pl.ds(mine, NU)]
    copy_to(sibling, DENS_SWAP, half, half).start()
    arrived_pair(DENS_SWAP, f_in.at[pl.ds(other, NU)])
    density = f_in[...].reshape(256, 128)
    weighted = coulexp[...] * density
    w_hi, w_lo = split(weighted)
    quarters = pk[...]

    def total_of(v):
        v = jnp.where(own128, v, 0.0)
        return fold(v[0:32] + v[32:64] + v[64:96] + v[96:128], 64, 32)

    exchange = total_of(dot(quarters, w_hi) + dot(quarters, w_lo))
    alpha_exchange = total_of(dot(density, weighted, 0, 0, precision=HIGH)) * (2.0 / NT / NT)
    x32 = x128[:, :32]
    base = ex128 + (2.0 / NT) * exchange - dot(x32, alpha_exchange, precision=HIGH)
    base = jnp.where(lane_is_t, base, 0.0)
    pick_m = iota((32, 8), 0)
    x_by_u = jnp.concatenate(
        [dot(x32, one_hot(pick_m == 4 * iota((32, 8), 1) + u), precision=HIGH) for u in range(4)],
        axis=0,
    )

    def four_blocks(v):
        v = jnp.where(own128, v, 0.0)
        return v[0:32] + v[32:64] + v[64:96] + v[96:128]

    arrived("col", ALPHA_COL, b_in)
    shares = jnp.sum(b_in[...], axis=0) * (1.0 / NT)
    projected = four_blocks(dot(x_by_u, shares, precision=HIGH))

    arrived("row", POT_ROW, y_in)
    direct = jnp.where(own64, dot(lk[...], y_in[...].reshape(512, 128)), 0.0)
    both = fold(projected + (direct[:32] + direct[32:]) * (1.0 / NK), 64, 32)
    rows = base - jnp.where(lane_is_t, both, 0.0)
    rows = rows + pltpu.roll(rows, 31, 0)
    rows = rows + pltpu.roll(rows, 30, 0)
    for i in range(8):
        at = 128 * (i % 4)
        out_ref[i // 4 : i // 4 + 1, at : at + 128] = rows[4 * i : 4 * i + 1, :]
    alpha = fold(jnp.where(lane_is_t, dot(spread, shares, precision=HIGH), 0.0), 64, 32)
    alpha_ref[...] = (alpha + alpha_exchange)[:, :32]

    for which, many in waits:
        wait_bytes(send_sems.at[which], many)


def on_device(pair_exchange, conduction, valence, coulomb, screening, energies, vectors, k_coords):
    q2, qa, qb, m_hi, m_lo = (jnp.asarray(table) for table in tables())
    operands = (
        *(pair_exchange, conduction, valence, coulomb.reshape(1, -1), energies, vectors, k_coords),
        *(q2, qa, qb, screening, m_hi, m_lo),
    )
    vmem = pl.BlockSpec(memory_space=pltpu.VMEM)
    return pl.pallas_call(
        kernel,
        out_shape=(
            jax.ShapeDtypeStruct((2, 512), F32),
            jax.ShapeDtypeStruct((32, 32), F32),
        ),
        in_specs=[pl.BlockSpec(memory_space=pltpu.HBM)] * len(operands),
        out_specs=(vmem, vmem),
        scratch_shapes=[
            pltpu.VMEM((2, 16, 1024), BF16),
            pltpu.VMEM((2, 4, 1024), BF16),
            pltpu.VMEM((2, 4, 1024), BF16),
            pltpu.VMEM((1, 1024), F32),
            pltpu.VMEM((2, 16), F32),
            pltpu.VMEM((2, 512), BF16),
            pltpu.SMEM((2, 2), jnp.int32),
            pltpu.VMEM((32, 64), BF16),
            pltpu.VMEM((64, NK), BF16),
            pltpu.VMEM((64, NK), BF16),
            pltpu.VMEM((8, 128), F32),
            pltpu.VMEM((32, 1024), F32),
            pltpu.VMEM((64, 512), BF16),
            pltpu.VMEM((128, 256), BF16),
            pltpu.VMEM((256, 128), F32),
            pltpu.VMEM((8, 256), F32),
            pltpu.VMEM((NR, NC, 128), BF16),
            pltpu.VMEM((NR, NC, 128), BF16),
            pltpu.VMEM((NC, NR, 128), BF16),
            pltpu.VMEM((NC, NR, 128), BF16),
            pltpu.VMEM((NC, NR, 128), BF16),
            pltpu.VMEM((NC, NR, 128), BF16),
            pltpu.VMEM((NR, NC, 128), BF16),
            pltpu.VMEM((NR, NC, 128), BF16),
            pltpu.VMEM((1, 128), F32),
            pltpu.VMEM((NR, 1, 128), F32),
            pltpu.VMEM((1, 128), F32),
            pltpu.VMEM((NC, 1, 128), F32),
            pltpu.VMEM((16, 128), F32),
            pltpu.VMEM((NR, 8, 128), F32),
            pltpu.VMEM((NU, 8, 128), F32),
            pltpu.VMEM((NU, 8, 128), F32),
            pltpu.VMEM((NU, 8, 128), F32),
            pltpu.VMEM((8, 128), F32),
            pltpu.VMEM((NC, 8, 128), F32),
            pltpu.VMEM((8, 128), F32),
            pltpu.VMEM((NR, 8, 128), F32),
            pltpu.VMEM((8, 128), BF16),
            pltpu.VMEM((NR, 8, 128), BF16),
            pltpu.VMEM((8, 128), F32),
            pltpu.VMEM((NC, 8, 128), F32),
            pltpu.VMEM((2, 32, 512), F32),
            pltpu.VMEM((2, 32, 512), F32),
            pltpu.VMEM((2048, NK), BF16),
            pltpu.VMEM((2, NK, 512), BF16),
            pltpu.VMEM((2, NK, 512), BF16),
            pltpu.VMEM((8, NK), F32),
            pltpu.VMEM((128, NK), BF16),
            pltpu.VMEM((128, 512), F32),
            pltpu.VMEM((512, 512), BF16),
            pltpu.VMEM((512, 512), BF16),
            pltpu.VMEM((2, QPAD, 128), F32),
            pltpu.VMEM((QPAD, NK), BF16),
            pltpu.VMEM((QPAD, NK), BF16),
            pltpu.SemaphoreType.DMA((13,)),
            pltpu.SemaphoreType.DMA((13,)),
            pltpu.SemaphoreType.DMA((14,)),
        ],
        compiler_params=pltpu.CompilerParams(
            collective_id=0, has_side_effects=True, vmem_limit_bytes=32 * 1024 * 1024
        ),
    )(*(pltpu.with_memory_space_constraint(v, pltpu.HBM) for v in operands))


def solution(mesh):
    split_k = ("row", "col")
    return jax.shard_map(
        on_device,
        mesh=mesh,
        in_specs=(
            P(split_k, None, None),
            P(split_k, None, None),
            P(split_k, None, None),
            P(),
            P(),
            P(split_k, None),
            P(split_k, None),
            P(split_k, None),
        ),
        out_specs=(P(split_k, None), P()),
        check_vma=False,
    )
```

```python
import jax
import jax.numpy as jnp
import numpy as np
from jax import lax
from jax.experimental import pallas as pl
from jax.experimental.pallas import tpu as pltpu
from jax.sharding import PartitionSpec as P

MESH = pl.DeviceIdType.MESH
HIGH = lax.Precision.HIGHEST
F32 = jnp.float32
BF16 = jnp.bfloat16

NR, NC, NU = 32, 16, 16
NK, NT = 1024, 16384
NQ = 289
QPAD = 384
COORD_ROW, COORD_COL, PROJ_ROW, PROJ_COL, POT_COL, POT_ROW = range(6)
DENS_PAIR, DENS_ROW, DENS_COL, DENS_OUT, DENS_SWAP = range(6, 11)
ALPHA_ROW, ALPHA_COL = range(11, 13)


def real_basis():
    points = np.arange(32)[None, :]
    order = np.arange(32)[:, None]
    freq = np.where(order <= 16, order, order - 16)
    angle = 2 * np.pi * freq * points / 32
    basis = np.where(order <= 16, np.cos(angle), np.sin(angle)) * np.sqrt(2 / 32)
    basis[[0, 16]] *= np.sqrt(0.5)
    return basis, freq[:, 0]


def two_parts(table):
    high = table.astype(BF16)
    return high, (table - high.astype(np.float64)).astype(BF16)


def tables():
    basis, freq = real_basis()
    fold = np.arange(17)
    weight = np.where((fold == 0) | (fold == 16), 1.0, 2.0)
    cosine = weight[None, :] * np.cos(2 * np.pi * freq[:, None] * fold[None, :] / 32)
    modes = np.zeros((QPAD, NK))
    modes[:NQ] = np.kron(cosine, cosine).T
    narrow = np.concatenate(two_parts(basis), axis=1)
    outer = np.concatenate(two_parts(np.repeat(basis.T, 32, axis=1)), axis=0)
    inner = np.concatenate(two_parts(np.tile(basis.T, (1, 32))), axis=0)
    return narrow, outer, inner, *two_parts(modes)


def iota(shape, dim):
    return lax.broadcasted_iota(jnp.int32, shape, dim)


def one_hot(mask):
    return jnp.where(mask, 1.0, 0.0).astype(F32)


def dot(a, b, ca=1, cb=0, precision=None):
    return lax.dot_general(
        a, b, (((ca,), (cb,)), ((), ())), precision=precision, preferred_element_type=F32
    )


def split(v):
    high = v.astype(BF16)
    return high, (v - high.astype(F32)).astype(BF16)


def fold(v, *shifts):
    for shift in shifts:
        v = v + pltpu.roll(v, shift, 1)
    return v


def kernel(
    pe_hbm, cond_hbm, val_hbm, coul_hbm, en_hbm, vec_hbm, kc_hbm, q2_hbm, qa_hbm, qb_hbm, scr_hbm,
    mhi_hbm, mlo_hbm,
    out_ref, alpha_ref,
    pe_ref, cond_ref, val_ref, coul_ref, en_ref, vec_ref, kc_ref, q2_ref, qa_ref, qb_ref,
    v8, pairs, lk, pk, coulexp, c8,
    p_out, p_in, q_out, q_in, z_out, z_in, y_out, y_in,
    k_out, k_in, h_out, h_in, c16,
    d_out, d_pair, d_sum, d_in, e_out, e_in, f_out, f_in,
    a_out, a_in, b_out, b_in,
    arow, brow, t_all, tt_hi, tt_lo, lam, wt, z_wide, perm_f, perm_b, scr, m_hi, m_lo,
    send_sems, recv_sems, local_sems,
):
    r, c = lax.axis_index("row"), lax.axis_index("col")
    core, chip = lax.rem(r, 2), r // 2
    groups = {"row": (NR, r), "col": (NC, c), "chip": (NU, chip)}

    def device(group, peer):
        if group == "chip":
            return {"row": 2 * peer + core}
        return {group: peer}

    z_at = [lax.rem(r // 4 + step, 8) for step in range(8)]
    near_at = [lax.rem(lax.rem(r, 4) + step, 4) for step in range(4)]
    y_lo_at = lax.rem(r, 4) // 2
    x_at = [lax.rem(c // 4 + step, 4) * 4 for step in range(4)]
    y_at = [lax.rem(lax.rem(c, 4) + step, 4) for step in range(4)]
    z_order = (4, 3, 5, 2, 6, 1, 7, 0)
    x_order = (2, 1, 3, 0)
    partners = {
        "row": [z_at[z] * 4 + near_at[n] for z in z_order for n in (1, 2, 3, 0)][:-1],
        "chip": [z_at[z] * 2 + y for z in z_order for y in (1 - y_lo_at, y_lo_at)][:-1],
        "col": [x_at[x] + y_at[2] for x in x_order]
        + [x_at[x] + y_at[y] for x in x_order for y in (1, 3)]
        + [x_at[x] + y_at[0] for x in x_order][:-1],
    }

    def peers(group, body):
        for peer in partners[group]:
            body(peer)

    def copy_to(device_id, which, source, target):
        return pltpu.make_async_remote_copy(
            src_ref=source,
            dst_ref=target,
            send_sem=send_sems.at[which],
            recv_sem=recv_sems.at[which],
            device_id=device_id,
            device_id_type=MESH,
        )

    def send(group, which, source, target, base=0):
        slot = base + groups[group][1]
        peers(
            group,
            lambda peer: copy_to(
                device(group, peer), which, source(peer), target.at[slot]
            ).start(),
        )

    def wait_bytes(sem, many):
        pltpu.make_async_copy(many, many, sem).wait()

    waits = []

    def arrived(group, which, target):
        many = target.at[pl.ds(0, groups[group][0] - 1)]
        waits.append((which, many))
        wait_bytes(recv_sems.at[which], many)

    def arrived_pair(which, target):
        waits.append((which, target))
        wait_bytes(recv_sems.at[which], target)

    sibling = {"row": r + 1 - 2 * core}

    barrier = pltpu.get_barrier_semaphore()
    for i in range(NR - 1):
        for axis in ("col", "row"):
            if i < groups[axis][0] - 1:
                there = {axis: partners[axis][i]}
                pl.semaphore_signal(barrier, inc=1, device_id=there, device_id_type=MESH)
    near = pl.multiple_of((r // 8) * 128, 128)
    far = pl.multiple_of((r // 8) * 128 + 512, 128)
    fetches = [
        pltpu.make_async_copy(source, target, local_sems.at[i])
        for i, (source, target) in enumerate(
            (
                (vec_hbm, vec_ref),
                (cond_hbm, cond_ref),
                (val_hbm, val_ref),
                (kc_hbm, kc_ref),
                (pe_hbm, pe_ref),
                (coul_hbm, coul_ref),
                (en_hbm, en_ref),
                (q2_hbm, q2_ref),
                (scr_hbm.at[:, pl.ds(near, 128)], scr.at[0, pl.ds(0, NQ), :]),
                (scr_hbm.at[:, pl.ds(far, 128)], scr.at[1, pl.ds(0, NQ), :]),
                (mhi_hbm, m_hi),
                (mlo_hbm, m_lo),
                (qa_hbm, qa_ref),
                (qb_hbm, qb_ref),
            )
        )
    ]
    for fetch in fetches:
        fetch.start()
    for fetch in fetches[:3]:
        fetch.wait()

    vec = vec_ref[...].astype(F32)
    for i in range(8):
        v8[i : i + 1, :] = vec[i // 4 : i // 4 + 1, (i % 4) * 128 : (i % 4 + 1) * 128]
    row32, lane32 = iota((32, 128), 0), iota((32, 128), 1)
    lane_is_t = (row32 & 3) == (lane32 >> 5)
    spread = one_hot((iota((32, 8), 0) >> 2) == iota((32, 8), 1))
    gather8 = one_hot((iota((8, 32), 1) >> 2) == iota((8, 32), 0))
    wide = dot(spread.astype(BF16), v8[...].astype(BF16))
    x128 = fold(jnp.where(lane_is_t, wide, 0.0), 64, 32)

    for k in range(2):
        cond = cond_ref[k].astype(F32)
        val = val_ref[k].astype(F32)
        for v in range(4):
            at = 16 * k + 4 * v
            pairs[at : at + 4, :] = val[v : v + 1, :] * cond
    pair_rows = pairs[...].astype(BF16)
    lk[0:32, :] = pair_rows[:, :512]
    lk[32:64, :] = pair_rows[:, 512:]
    row64, lane64 = iota((64, 128), 0), iota((64, 128), 1)
    own64 = ((row64 >> 5) == ((lane64 >> 5) & 1)) & (((row64 >> 4) & 1) == (lane64 >> 6))
    x_block = jnp.where(own64, jnp.concatenate([x128, x128], axis=0), 0.0).astype(BF16)
    p_out[...] = dot(lk[...], x_block, 0, 0).astype(BF16).reshape(NR, NC, 128)

    for fetch in fetches[3:8]:
        fetch.wait()
    place = iota((1, 128), 1) - 4 * r
    k_row = jnp.zeros((1, 128), jnp.int32)
    for q in range(4):
        k_row = jnp.where(place == q, kc_ref[q // 2, q % 2], k_row)
    k_out[...] = k_row.astype(F32)

    pl.semaphore_wait(barrier, NR + NC - 2)
    send("row", COORD_ROW, lambda peer: k_out, k_in)
    send("row", PROJ_ROW, lambda peer: p_out.at[peer], p_in)
    k_in[pl.ds(r, 1)] = k_out[...].reshape(1, 1, 128)
    p_in[pl.ds(r, 1)] = p_out[pl.ds(r, 1)]

    for k in range(2):
        for j in range(4):
            at = 32 * j + 16 * k
            pk[at : at + 16, :] = pe_ref[k, :, j * 256 : (j + 1) * 256]
    own128 = (iota((128, 128), 0) >> 5) == (iota((128, 128), 1) >> 5)
    x_quarter = jnp.where(own128, jnp.concatenate([x128] * 4, axis=0), 0.0).astype(BF16)
    d_out[...] = dot(pk[...], x_quarter, 0, 0).reshape(NR, 8, 128)
    mine = pl.multiple_of(core * NU, NU)
    other = pl.multiple_of(NU - core * NU, NU)
    copy_to(sibling, DENS_PAIR, d_out.at[pl.ds(other, NU)], d_pair).start()

    def build_perm(i, carry):
        at = pl.multiple_of(i * 128, 128)
        row, col = iota((128, 512), 0) + i * 128, iota((128, 512), 1)
        perm_f[pl.ds(at, 128), :] = one_hot(col == ((row & 31) << 4) + (row >> 5)).astype(BF16)
        perm_b[pl.ds(at, 128), :] = one_hot(col == ((row & 15) << 5) + (row >> 4)).astype(BF16)
        return carry

    lax.fori_loop(0, 4, build_perm, 0)

    arrived_pair(DENS_PAIR, d_pair)
    d_sum[...] = d_out[pl.ds(mine, NU)] + d_pair[...]
    send("chip", DENS_ROW, lambda peer: d_sum.at[peer], d_in)
    d_in[pl.ds(chip, 1)] = d_sum[pl.ds(chip, 1)]

    energy = jnp.concatenate(
        [jnp.broadcast_to(en_ref[k : k + 1, :], (16, 16)) for k in range(2)], axis=0
    )
    same = (iota((32, 16), 0) & 15) == iota((32, 16), 1)
    e_col = jnp.sum(jnp.where(same, energy, 0.0), axis=1, keepdims=True)
    ex128 = e_col * x128
    alpha_energy = dot(x128, ex128, 0, 0, precision=HIGH)[:32]

    for fetch in fetches[8:]:
        fetch.wait()
    chosen = lax.rem(r, 8) * 16 + c
    q_row, q_lane = iota((8, 128), 0), iota((8, 128), 1)
    known = iota((QPAD, 128), 0) < NQ
    values = sum(
        dot(
            one_hot((q_row == h) & (q_lane == chosen)),
            jnp.where(known, scr[h], 0.0),
            1,
            1,
            precision=HIGH,
        )
        for h in range(2)
    )
    s_hi, s_lo = split(values)
    lam[...] = dot(s_hi, m_hi[...]) + dot(s_lo, m_hi[...]) + dot(s_hi, m_lo[...])

    arrived("row", COORD_ROW, k_in)
    h_out[...] = jnp.sum(k_in[...], axis=0)
    send("col", COORD_COL, lambda peer: h_out, h_in)
    h_in[pl.ds(c, 1)] = h_out[...].reshape(1, 1, 128)

    arrived("row", PROJ_ROW, p_in)
    mixed = dot(perm_f[...], p_in[...].reshape(512, 128)).astype(BF16)
    q_out[...] = mixed.reshape(NC, NR, 128)
    send("col", PROJ_COL, lambda peer: q_out.at[peer], q_in)
    q_in[pl.ds(c, 1)] = q_out[pl.ds(c, 1)]
    arrived("chip", DENS_ROW, d_in)
    e_out[...] = jnp.sum(d_in[...], axis=0)
    send("col", DENS_COL, lambda peer: e_out, e_in)
    e_in[pl.ds(c, 1)] = e_out[...].reshape(1, 8, 128)

    arrived("col", COORD_COL, h_in)
    for i in range(NC):
        c16[i : i + 1, :] = h_in[i]
    repeat = one_hot(iota((16, 512), 0) == (iota((16, 512), 1) >> 5)).astype(BF16)
    spread_c = dot(c16[...].astype(BF16), repeat, 0, 0)
    row128, lane512 = iota((128, 512), 0), iota((128, 512), 1)
    kept = jnp.where((row128 >> 2) == (lane512 & 31), spread_c, 0.0).astype(BF16)
    pick = one_hot((iota((128, 128), 0) >> 5) == (iota((128, 128), 1) & 3)).astype(BF16)
    coords = dot(pick, kept)
    hot = one_hot(coords == (row128 & 31).astype(F32)).astype(BF16)
    q2 = q2_ref[...]
    for k in range(2):
        at = 64 * k
        first = jnp.concatenate([hot[at : at + 32]] * 2, axis=0)
        second = jnp.concatenate([hot[at + 32 : at + 64]] * 2, axis=0)
        arow[k] = dot(q2, first)
        brow[k] = dot(q2, second)
        for i in range(4):
            at = 128 * i
            outer = dot(first[:, at : at + 128], qa_ref[...], 0, 0)
            inner = dot(second[:, at : at + 128], qb_ref[...], 0, 0)
            high, low = split(outer * inner)
            t_all[512 * k + at : 512 * k + at + 128, :] = high
            t_all[1024 + 512 * k + at : 1024 + 512 * k + at + 128, :] = low

    def build_basis(j, carry):
        at = pl.multiple_of(j * 32, 32)
        for k in range(2):
            high, low = split(arow[k, pl.ds(j, 1), :] * brow[k])
            tt_hi[k, pl.ds(at, 32), :] = high
            tt_lo[k, pl.ds(at, 32), :] = low
        return carry

    lax.fori_loop(0, 32, build_basis, 0)

    arrived("col", PROJ_COL, q_in)
    turned = jnp.transpose(q_in[...].reshape(512, 128).astype(F32)).astype(BF16)
    mode = dot(jnp.concatenate([turned[:64], turned[64:]] * 2, axis=1), t_all[...])
    first_g = iota((64, NK), 0) < 32
    scaled = jnp.where(first_g, lam[0:1, :], lam[1:2, :]) * mode
    high, low = split(scaled)
    wt[0:64, :] = high
    wt[64:128, :] = low
    alpha_direct = dot(mode.astype(BF16), jnp.concatenate([high, high], axis=0), 1, 1)
    kept_g = jnp.where((row64 >> 5) == ((lane64 >> 5) & 1), alpha_direct, 0.0)
    part = alpha_energy - fold(kept_g[:32] + kept_g[32:], 32) * (1.0 / NK)
    packed = dot(gather8, jnp.where(lane_is_t, part, 0.0), precision=HIGH)
    a_out[...] = packed.astype(BF16)

    for k in range(2):
        both = dot(wt[...], tt_hi[k])
        back = both[:64] + both[64:] + dot(wt[0:64, :], tt_lo[k])
        z_wide[64 * k : 64 * k + 64, :] = back
    z_out[...] = jnp.transpose(z_wide[...]).astype(BF16).reshape(NC, NR, 128)
    send("col", POT_COL, lambda peer: z_out.at[peer], z_in)
    z_in[pl.ds(c, 1)] = z_out[pl.ds(c, 1)]

    send("row", ALPHA_ROW, lambda peer: a_out, a_in)
    a_in[pl.ds(r, 1)] = a_out[...].reshape(1, 8, 128)

    arrived("col", DENS_COL, e_in)
    f_out[...] = jnp.sum(e_in[...], axis=0)
    send("chip", DENS_OUT, lambda peer: f_out, f_in, base=mine)
    f_in[pl.ds(mine + chip, 1)] = f_out[...].reshape(1, 8, 128)

    c8[...] = jnp.zeros((8, 256), F32)
    for j in range(4):
        c8[j : j + 1, :] = coul_ref[:, j * 256 : (j + 1) * 256]
    expand8 = one_hot(iota((8, 128), 0) == (iota((8, 128), 1) >> 5))
    coulexp[...] = dot(c8[...], expand8, 0, 0, precision=HIGH)

    arrived("col", POT_COL, z_in)
    mixed = dot(perm_b[...], z_in[...].reshape(512, 128)).astype(BF16)
    y_out[...] = mixed.reshape(NR, NC, 128)
    send("row", POT_ROW, lambda peer: y_out.at[peer], y_in)
    y_in[pl.ds(r, 1)] = y_out[pl.ds(r, 1)]

    arrived("row", ALPHA_ROW, a_in)
    b_out[...] = jnp.sum(a_in[...].astype(F32), axis=0)
    send("col", ALPHA_COL, lambda peer: b_out, b_in)
    b_in[pl.ds(c, 1)] = b_out[...].reshape(1, 8, 128)

    arrived("chip", DENS_OUT, f_in)
    half = f_in.at[pl.ds(mine, NU)]
    copy_to(sibling, DENS_SWAP, half, half).start()
    arrived_pair(DENS_SWAP, f_in.at[pl.ds(other, NU)])
    density = f_in[...].reshape(256, 128)
    weighted = coulexp[...] * density
    w_hi, w_lo = split(weighted)
    quarters = pk[...]

    def total_of(v):
        v = jnp.where(own128, v, 0.0)
        return fold(v[0:32] + v[32:64] + v[64:96] + v[96:128], 64, 32)

    exchange = total_of(dot(quarters, w_hi) + dot(quarters, w_lo))
    alpha_exchange = total_of(dot(density, weighted, 0, 0, precision=HIGH)) * (2.0 / NT / NT)
    x32 = x128[:, :32]
    base = ex128 + (2.0 / NT) * exchange - dot(x32, alpha_exchange, precision=HIGH)
    base = jnp.where(lane_is_t, base, 0.0)
    pick_m = iota((32, 8), 0)
    x_by_u = jnp.concatenate(
        [dot(x32, one_hot(pick_m == 4 * iota((32, 8), 1) + u), precision=HIGH) for u in range(4)],
        axis=0,
    )

    def four_blocks(v):
        v = jnp.where(own128, v, 0.0)
        return v[0:32] + v[32:64] + v[64:96] + v[96:128]

    arrived("col", ALPHA_COL, b_in)
    shares = jnp.sum(b_in[...], axis=0) * (1.0 / NT)
    projected = four_blocks(dot(x_by_u, shares, precision=HIGH))

    arrived("row", POT_ROW, y_in)
    direct = jnp.where(own64, dot(lk[...], y_in[...].reshape(512, 128)), 0.0)
    both = fold(projected + (direct[:32] + direct[32:]) * (1.0 / NK), 64, 32)
    rows = base - jnp.where(lane_is_t, both, 0.0)
    rows = rows + pltpu.roll(rows, 31, 0)
    rows = rows + pltpu.roll(rows, 30, 0)
    for i in range(8):
        at = 128 * (i % 4)
        out_ref[i // 4 : i // 4 + 1, at : at + 128] = rows[4 * i : 4 * i + 1, :]
    alpha = fold(jnp.where(lane_is_t, dot(spread, shares, precision=HIGH), 0.0), 64, 32)
    alpha_ref[...] = (alpha + alpha_exchange)[:, :32]

    for which, many in waits:
        wait_bytes(send_sems.at[which], many)


def on_device(pair_exchange, conduction, valence, coulomb, screening, energies, vectors, k_coords):
    q2, qa, qb, m_hi, m_lo = (jnp.asarray(table) for table in tables())
    operands = (
        *(pair_exchange, conduction, valence, coulomb.reshape(1, -1), energies, vectors, k_coords),
        *(q2, qa, qb, screening, m_hi, m_lo),
    )
    vmem = pl.BlockSpec(memory_space=pltpu.VMEM)
    return pl.pallas_call(
        kernel,
        out_shape=(
            jax.ShapeDtypeStruct((2, 512), F32),
            jax.ShapeDtypeStruct((32, 32), F32),
        ),
        in_specs=[pl.BlockSpec(memory_space=pltpu.HBM)] * len(operands),
        out_specs=(vmem, vmem),
        scratch_shapes=[
            pltpu.VMEM((2, 16, 1024), BF16),
            pltpu.VMEM((2, 4, 1024), BF16),
            pltpu.VMEM((2, 4, 1024), BF16),
            pltpu.VMEM((1, 1024), F32),
            pltpu.VMEM((2, 16), F32),
            pltpu.VMEM((2, 512), BF16),
            pltpu.SMEM((2, 2), jnp.int32),
            pltpu.VMEM((32, 64), BF16),
            pltpu.VMEM((64, NK), BF16),
            pltpu.VMEM((64, NK), BF16),
            pltpu.VMEM((8, 128), F32),
            pltpu.VMEM((32, 1024), F32),
            pltpu.VMEM((64, 512), BF16),
            pltpu.VMEM((128, 256), BF16),
            pltpu.VMEM((256, 128), F32),
            pltpu.VMEM((8, 256), F32),
            pltpu.VMEM((NR, NC, 128), BF16),
            pltpu.VMEM((NR, NC, 128), BF16),
            pltpu.VMEM((NC, NR, 128), BF16),
            pltpu.VMEM((NC, NR, 128), BF16),
            pltpu.VMEM((NC, NR, 128), BF16),
            pltpu.VMEM((NC, NR, 128), BF16),
            pltpu.VMEM((NR, NC, 128), BF16),
            pltpu.VMEM((NR, NC, 128), BF16),
            pltpu.VMEM((1, 128), F32),
            pltpu.VMEM((NR, 1, 128), F32),
            pltpu.VMEM((1, 128), F32),
            pltpu.VMEM((NC, 1, 128), F32),
            pltpu.VMEM((16, 128), F32),
            pltpu.VMEM((NR, 8, 128), F32),
            pltpu.VMEM((NU, 8, 128), F32),
            pltpu.VMEM((NU, 8, 128), F32),
            pltpu.VMEM((NU, 8, 128), F32),
            pltpu.VMEM((8, 128), F32),
            pltpu.VMEM((NC, 8, 128), F32),
            pltpu.VMEM((8, 128), F32),
            pltpu.VMEM((NR, 8, 128), F32),
            pltpu.VMEM((8, 128), BF16),
            pltpu.VMEM((NR, 8, 128), BF16),
            pltpu.VMEM((8, 128), F32),
            pltpu.VMEM((NC, 8, 128), F32),
            pltpu.VMEM((2, 32, 512), F32),
            pltpu.VMEM((2, 32, 512), F32),
            pltpu.VMEM((2048, NK), BF16),
            pltpu.VMEM((2, NK, 512), BF16),
            pltpu.VMEM((2, NK, 512), BF16),
            pltpu.VMEM((8, NK), F32),
            pltpu.VMEM((128, NK), BF16),
            pltpu.VMEM((128, 512), F32),
            pltpu.VMEM((512, 512), BF16),
            pltpu.VMEM((512, 512), BF16),
            pltpu.VMEM((2, QPAD, 128), F32),
            pltpu.VMEM((QPAD, NK), BF16),
            pltpu.VMEM((QPAD, NK), BF16),
            pltpu.SemaphoreType.DMA((13,)),
            pltpu.SemaphoreType.DMA((13,)),
            pltpu.SemaphoreType.DMA((14,)),
        ],
        compiler_params=pltpu.CompilerParams(
            collective_id=0, has_side_effects=True, vmem_limit_bytes=32 * 1024 * 1024
        ),
    )(*(pltpu.with_memory_space_constraint(v, pltpu.HBM) for v in operands))


def solution(mesh):
    split_k = ("row", "col")
    return jax.shard_map(
        on_device,
        mesh=mesh,
        in_specs=(
            P(split_k, None, None),
            P(split_k, None, None),
            P(split_k, None, None),
            P(),
            P(),
            P(split_k, None),
            P(split_k, None),
            P(split_k, None),
        ),
        out_specs=(P(split_k, None), P()),
        check_vma=False,
    )
```

```python
import jax
import jax.numpy as jnp
import numpy as np
from jax import lax
from jax.experimental import pallas as pl
from jax.experimental.pallas import tpu as pltpu
from jax.sharding import PartitionSpec as P

MESH = pl.DeviceIdType.MESH
HIGH = lax.Precision.HIGHEST
F32 = jnp.float32
BF16 = jnp.bfloat16

NR, NC, NU = 32, 16, 16
NK, NT = 1024, 16384
NQ = 289
QPAD = 384
EARLY = 16
COORD_ROW, COORD_COL, PROJ_ROW, PROJ_COL, POT_COL, POT_ROW = range(6)
DENS_PAIR, DENS_ROW, DENS_COL, DENS_OUT, DENS_SWAP = range(6, 11)
ALPHA_ROW, ALPHA_COL = range(11, 13)


def real_basis():
    points = np.arange(32)[None, :]
    order = np.arange(32)[:, None]
    freq = np.where(order <= 16, order, order - 16)
    angle = 2 * np.pi * freq * points / 32
    basis = np.where(order <= 16, np.cos(angle), np.sin(angle)) * np.sqrt(2 / 32)
    basis[[0, 16]] *= np.sqrt(0.5)
    return basis, freq[:, 0]


def two_parts(table):
    high = table.astype(BF16)
    return high, (table - high.astype(np.float64)).astype(BF16)


def tables():
    basis, freq = real_basis()
    fold = np.arange(17)
    weight = np.where((fold == 0) | (fold == 16), 1.0, 2.0)
    cosine = weight[None, :] * np.cos(2 * np.pi * freq[:, None] * fold[None, :] / 32)
    modes = np.zeros((QPAD, NK))
    modes[:NQ] = np.kron(cosine, cosine).T
    narrow = np.concatenate(two_parts(basis), axis=1)
    outer = np.concatenate(two_parts(np.repeat(basis.T, 32, axis=1)), axis=0)
    inner = np.concatenate(two_parts(np.tile(basis.T, (1, 32))), axis=0)
    return narrow, outer, inner, *two_parts(modes)


def iota(shape, dim):
    return lax.broadcasted_iota(jnp.int32, shape, dim)


def one_hot(mask):
    return jnp.where(mask, 1.0, 0.0).astype(F32)


def dot(a, b, ca=1, cb=0, precision=None):
    return lax.dot_general(
        a, b, (((ca,), (cb,)), ((), ())), precision=precision, preferred_element_type=F32
    )


def split(v):
    high = v.astype(BF16)
    return high, (v - high.astype(F32)).astype(BF16)


def fold(v, *shifts):
    for shift in shifts:
        v = v + pltpu.roll(v, shift, 1)
    return v


def kernel(
    pe_hbm, cond_hbm, val_hbm, coul_hbm, en_hbm, vec_hbm, kc_hbm, q2_hbm, qa_hbm, qb_hbm, scr_hbm,
    mhi_hbm, mlo_hbm,
    out_ref, alpha_ref,
    pe_ref, cond_ref, val_ref, coul_ref, en_ref, vec_ref, kc_ref, q2_ref, qa_ref, qb_ref,
    v8, pairs, lk, pk, coulexp, c8,
    p_out, p_in, q_out, q_in, z_out, z_in, y_out, y_in,
    k_out, k_in, h_out, h_in, c16,
    d_out, d_pair, d_sum, d_in, e_out, e_in, f_out, f_in,
    a_out, a_in, b_out, b_in,
    arow, brow, t_all, tt_hi, tt_lo, lam, modes, wt, z_wide, perm_f, perm_b, scr, m_hi, m_lo,
    send_sems, recv_sems, local_sems,
):
    r, c = lax.axis_index("row"), lax.axis_index("col")
    core, chip = lax.rem(r, 2), r // 2
    groups = {"row": (NR, r), "col": (NC, c), "chip": (NU, chip)}

    def device(group, peer):
        if group == "chip":
            return {"row": 2 * peer + core}
        return {group: peer}

    z_at = [lax.rem(r // 4 + step, 8) for step in range(8)]
    near_at = [lax.rem(lax.rem(r, 4) + step, 4) for step in range(4)]
    y_lo_at = lax.rem(r, 4) // 2
    x_at = [lax.rem(c // 4 + step, 4) * 4 for step in range(4)]
    y_at = [lax.rem(lax.rem(c, 4) + step, 4) for step in range(4)]
    z_order = (4, 3, 5, 2, 6, 1, 7, 0)
    x_order = (2, 1, 3, 0)
    partners = {
        "row": [z_at[z] * 4 + near_at[n] for z in z_order for n in (1, 2, 3, 0)][:-1],
        "chip": [z_at[z] * 2 + y for z in z_order for y in (1 - y_lo_at, y_lo_at)][:-1],
        "col": [x_at[x] + y_at[2] for x in x_order]
        + [x_at[x] + y_at[y] for x in x_order for y in (1, 3)]
        + [x_at[x] + y_at[0] for x in x_order][:-1],
    }

    def peers(group, body):
        for peer in partners[group]:
            body(peer)

    def copy_to(device_id, which, source, target):
        return pltpu.make_async_remote_copy(
            src_ref=source,
            dst_ref=target,
            send_sem=send_sems.at[which],
            recv_sem=recv_sems.at[which],
            device_id=device_id,
            device_id_type=MESH,
        )

    def send(group, which, source, target, base=0):
        slot = base + groups[group][1]
        peers(
            group,
            lambda peer: copy_to(
                device(group, peer), which, source(peer), target.at[slot]
            ).start(),
        )

    def wait_bytes(sem, many):
        pltpu.make_async_copy(many, many, sem).wait()

    waits = []

    def arrived(group, which, target):
        many = target.at[pl.ds(0, groups[group][0] - 1)]
        waits.append((which, many))
        wait_bytes(recv_sems.at[which], many)

    def arrived_pair(which, target):
        waits.append((which, target))
        wait_bytes(recv_sems.at[which], target)

    sibling = {"row": r + 1 - 2 * core}

    barrier = pltpu.get_barrier_semaphore()
    for i in range(NR - 1):
        for axis in ("col", "row"):
            if i < groups[axis][0] - 1:
                there = {axis: partners[axis][i]}
                pl.semaphore_signal(barrier, inc=1, device_id=there, device_id_type=MESH)
    near = pl.multiple_of((r // 8) * 128, 128)
    far = pl.multiple_of((r // 8) * 128 + 512, 128)
    fetches = [
        pltpu.make_async_copy(source, target, local_sems.at[i])
        for i, (source, target) in enumerate(
            (
                (vec_hbm, vec_ref),
                (cond_hbm, cond_ref),
                (val_hbm, val_ref),
                (kc_hbm, kc_ref),
                (pe_hbm, pe_ref),
                (coul_hbm, coul_ref),
                (en_hbm, en_ref),
                (q2_hbm, q2_ref),
                (scr_hbm.at[:, pl.ds(near, 128)], scr.at[0, pl.ds(0, NQ), :]),
                (scr_hbm.at[:, pl.ds(far, 128)], scr.at[1, pl.ds(0, NQ), :]),
                (mhi_hbm, m_hi),
                (mlo_hbm, m_lo),
                (qa_hbm, qa_ref),
                (qb_hbm, qb_ref),
            )
        )
    ]
    for fetch in fetches:
        fetch.start()
    for fetch in fetches[:3]:
        fetch.wait()

    vec = vec_ref[...].astype(F32)
    for i in range(8):
        v8[i : i + 1, :] = vec[i // 4 : i // 4 + 1, (i % 4) * 128 : (i % 4 + 1) * 128]
    row32, lane32 = iota((32, 128), 0), iota((32, 128), 1)
    lane_is_t = (row32 & 3) == (lane32 >> 5)
    spread = one_hot((iota((32, 8), 0) >> 2) == iota((32, 8), 1))
    gather8 = one_hot((iota((8, 32), 1) >> 2) == iota((8, 32), 0))
    wide = dot(spread.astype(BF16), v8[...].astype(BF16))
    x128 = fold(jnp.where(lane_is_t, wide, 0.0), 64, 32)

    for k in range(2):
        cond = cond_ref[k].astype(F32)
        val = val_ref[k].astype(F32)
        for v in range(4):
            at = 16 * k + 4 * v
            pairs[at : at + 4, :] = val[v : v + 1, :] * cond
    pair_rows = pairs[...].astype(BF16)
    lk[0:32, :] = pair_rows[:, :512]
    lk[32:64, :] = pair_rows[:, 512:]
    row64, lane64 = iota((64, 128), 0), iota((64, 128), 1)
    own64 = ((row64 >> 5) == ((lane64 >> 5) & 1)) & (((row64 >> 4) & 1) == (lane64 >> 6))
    x_block = jnp.where(own64, jnp.concatenate([x128, x128], axis=0), 0.0).astype(BF16)
    p_out[...] = dot(lk[...], x_block, 0, 0).astype(BF16).reshape(NR, NC, 128)

    for fetch in fetches[3:8]:
        fetch.wait()
    place = iota((1, 128), 1) - 4 * r
    k_row = jnp.zeros((1, 128), jnp.int32)
    for q in range(4):
        k_row = jnp.where(place == q, kc_ref[q // 2, q % 2], k_row)
    k_out[...] = k_row.astype(F32)

    pl.semaphore_wait(barrier, NR + NC - 2)
    send("row", COORD_ROW, lambda peer: k_out, k_in)
    send("row", PROJ_ROW, lambda peer: p_out.at[peer], p_in)
    k_in[pl.ds(r, 1)] = k_out[...].reshape(1, 1, 128)
    p_in[pl.ds(r, 1)] = p_out[pl.ds(r, 1)]

    for k in range(2):
        for j in range(4):
            at = 32 * j + 16 * k
            pk[at : at + 16, :] = pe_ref[k, :, j * 256 : (j + 1) * 256]
    own128 = (iota((128, 128), 0) >> 5) == (iota((128, 128), 1) >> 5)
    x_quarter = jnp.where(own128, jnp.concatenate([x128] * 4, axis=0), 0.0).astype(BF16)
    d_out[...] = dot(pk[...], x_quarter, 0, 0).reshape(NR, 8, 128)
    mine = pl.multiple_of(core * NU, NU)
    other = pl.multiple_of(NU - core * NU, NU)
    copy_to(sibling, DENS_PAIR, d_out.at[pl.ds(other, NU)], d_pair).start()

    def build_perm(i, carry):
        at = pl.multiple_of(i * 128, 128)
        row, col = iota((128, 512), 0) + i * 128, iota((128, 512), 1)
        perm_f[pl.ds(at, 128), :] = one_hot(col == ((row & 31) << 4) + (row >> 5)).astype(BF16)
        perm_b[pl.ds(at, 128), :] = one_hot(col == ((row & 15) << 5) + (row >> 4)).astype(BF16)
        return carry

    lax.fori_loop(0, 4, build_perm, 0)

    arrived_pair(DENS_PAIR, d_pair)
    d_sum[...] = d_out[pl.ds(mine, NU)] + d_pair[...]
    send("chip", DENS_ROW, lambda peer: d_sum.at[peer], d_in)
    d_in[pl.ds(chip, 1)] = d_sum[pl.ds(chip, 1)]

    energy = jnp.concatenate(
        [jnp.broadcast_to(en_ref[k : k + 1, :], (16, 16)) for k in range(2)], axis=0
    )
    same = (iota((32, 16), 0) & 15) == iota((32, 16), 1)
    e_col = jnp.sum(jnp.where(same, energy, 0.0), axis=1, keepdims=True)
    ex128 = e_col * x128
    alpha_energy = dot(x128, ex128, 0, 0, precision=HIGH)[:32]

    for fetch in fetches[8:]:
        fetch.wait()
    chosen = lax.rem(r, 8) * 16 + c
    q_row, q_lane = iota((8, 128), 0), iota((8, 128), 1)
    known = iota((QPAD, 128), 0) < NQ
    values = sum(
        dot(
            one_hot((q_row == h) & (q_lane == chosen)),
            jnp.where(known, scr[h], 0.0),
            1,
            1,
            precision=HIGH,
        )
        for h in range(2)
    )
    s_hi, s_lo = split(values)
    lam[...] = dot(s_hi, m_hi[...]) + dot(s_lo, m_hi[...]) + dot(s_hi, m_lo[...])

    arrived("row", COORD_ROW, k_in)
    h_out[...] = jnp.sum(k_in[...], axis=0)
    send("col", COORD_COL, lambda peer: h_out, h_in)
    h_in[pl.ds(c, 1)] = h_out[...].reshape(1, 1, 128)

    arrived("row", PROJ_ROW, p_in)
    mixed = dot(perm_f[...], p_in[...].reshape(512, 128)).astype(BF16)
    q_out[...] = mixed.reshape(NC, NR, 128)
    send("col", PROJ_COL, lambda peer: q_out.at[peer], q_in)
    q_in[pl.ds(c, 1)] = q_out[pl.ds(c, 1)]
    arrived("chip", DENS_ROW, d_in)
    e_out[...] = jnp.sum(d_in[...], axis=0)
    send("col", DENS_COL, lambda peer: e_out, e_in)
    e_in[pl.ds(c, 1)] = e_out[...].reshape(1, 8, 128)

    arrived("col", COORD_COL, h_in)
    for i in range(NC):
        c16[i : i + 1, :] = h_in[i]
    repeat = one_hot(iota((16, 512), 0) == (iota((16, 512), 1) >> 5)).astype(BF16)
    spread_c = dot(c16[...].astype(BF16), repeat, 0, 0)
    row128, lane512 = iota((128, 512), 0), iota((128, 512), 1)
    kept = jnp.where((row128 >> 2) == (lane512 & 31), spread_c, 0.0).astype(BF16)
    pick = one_hot((iota((128, 128), 0) >> 5) == (iota((128, 128), 1) & 3)).astype(BF16)
    coords = dot(pick, kept)
    hot = one_hot(coords == (row128 & 31).astype(F32)).astype(BF16)
    q2 = q2_ref[...]
    for k in range(2):
        at = 64 * k
        first = jnp.concatenate([hot[at : at + 32]] * 2, axis=0)
        second = jnp.concatenate([hot[at + 32 : at + 64]] * 2, axis=0)
        arow[k] = dot(q2, first)
        brow[k] = dot(q2, second)
        for i in range(4):
            at = 128 * i
            outer = dot(first[:, at : at + 128], qa_ref[...], 0, 0)
            inner = dot(second[:, at : at + 128], qb_ref[:, :128], 0, 0)
            for b in range(8):
                high, low = split(outer[:, 128 * b : 128 * b + 128] * inner)
                lanes = slice(128 * b, 128 * b + 128)
                t_all[512 * k + at : 512 * k + at + 128, lanes] = high
                t_all[1024 + 512 * k + at : 1024 + 512 * k + at + 128, lanes] = low

    def turn_basis(outer_modes):
        for j in outer_modes:
            for k in range(2):
                high, low = split(arow[k, j : j + 1, :] * brow[k])
                tt_hi[k, 32 * j : 32 * j + 32, :] = high
                tt_lo[k, 32 * j : 32 * j + 32, :] = low

    turn_basis(range(EARLY))

    arrived("col", PROJ_COL, q_in)
    turned = jnp.transpose(q_in[...].reshape(512, 128).astype(F32)).astype(BF16)
    turned = jnp.concatenate([turned[:64], turned[64:]] * 2, axis=1)
    first_g = iota((64, 256), 0) < 32
    for i in range(4):
        lanes = slice(256 * i, 256 * i + 256)
        mode = dot(turned, t_all[:, lanes])
        turn_basis(range(EARLY + (32 - EARLY) // 4 * i, EARLY + (32 - EARLY) // 4 * (i + 1)))
        high, low = split(jnp.where(first_g, lam[0:1, lanes], lam[1:2, lanes]) * mode)
        modes[:, lanes] = mode.astype(BF16)
        wt[0:64, lanes] = high
        wt[64:128, lanes] = low

    for k in range(2):
        both = dot(wt[...], tt_hi[k])
        back = both[:64] + both[64:] + dot(wt[0:64, :], tt_lo[k])
        z_wide[64 * k : 64 * k + 64, :] = back
    z_out[...] = jnp.transpose(z_wide[...]).astype(BF16).reshape(NC, NR, 128)
    send("col", POT_COL, lambda peer: z_out.at[peer], z_in)
    z_in[pl.ds(c, 1)] = z_out[pl.ds(c, 1)]

    high = wt[0:64, :]
    alpha_direct = dot(modes[...], jnp.concatenate([high, high], axis=0), 1, 1)
    kept_g = jnp.where((row64 >> 5) == ((lane64 >> 5) & 1), alpha_direct, 0.0)
    part = alpha_energy - fold(kept_g[:32] + kept_g[32:], 32) * (1.0 / NK)
    part = jnp.where(lane_is_t, part, 0.0).astype(BF16)
    a_out[...] = dot(gather8.astype(BF16), part).astype(BF16)
    send("row", ALPHA_ROW, lambda peer: a_out, a_in)
    a_in[pl.ds(r, 1)] = a_out[...].reshape(1, 8, 128)

    arrived("col", DENS_COL, e_in)
    f_out[...] = jnp.sum(e_in[...], axis=0)
    send("chip", DENS_OUT, lambda peer: f_out, f_in, base=mine)
    f_in[pl.ds(mine + chip, 1)] = f_out[...].reshape(1, 8, 128)

    c8[...] = jnp.zeros((8, 256), F32)
    for j in range(4):
        c8[j : j + 1, :] = coul_ref[:, j * 256 : (j + 1) * 256]
    expand8 = one_hot(iota((8, 128), 0) == (iota((8, 128), 1) >> 5))
    coulexp[...] = dot(c8[...], expand8, 0, 0, precision=HIGH)

    arrived("col", POT_COL, z_in)
    mixed = dot(perm_b[...], z_in[...].reshape(512, 128)).astype(BF16)
    y_out[...] = mixed.reshape(NR, NC, 128)
    send("row", POT_ROW, lambda peer: y_out.at[peer], y_in)
    y_in[pl.ds(r, 1)] = y_out[pl.ds(r, 1)]

    arrived("row", ALPHA_ROW, a_in)
    b_out[...] = jnp.sum(a_in[...].astype(F32), axis=0)
    send("col", ALPHA_COL, lambda peer: b_out, b_in)
    b_in[pl.ds(c, 1)] = b_out[...].reshape(1, 8, 128)

    arrived("chip", DENS_OUT, f_in)
    half = f_in.at[pl.ds(mine, NU)]
    copy_to(sibling, DENS_SWAP, half, half).start()
    arrived_pair(DENS_SWAP, f_in.at[pl.ds(other, NU)])
    density = f_in[...].reshape(256, 128)
    weighted = coulexp[...] * density
    w_hi, w_lo = split(weighted)
    quarters = pk[...]

    def total_of(v):
        v = jnp.where(own128, v, 0.0)
        return fold(v[0:32] + v[32:64] + v[64:96] + v[96:128], 64, 32)

    exchange = total_of(dot(quarters, w_hi) + dot(quarters, w_lo))
    alpha_exchange = total_of(dot(density, weighted, 0, 0, precision=HIGH)) * (2.0 / NT / NT)
    x32 = x128[:, :32]
    base = ex128 + (2.0 / NT) * exchange - dot(x32, alpha_exchange, precision=HIGH)
    base = jnp.where(lane_is_t, base, 0.0)
    pick_m = iota((32, 8), 0)
    x_by_u = jnp.concatenate(
        [dot(x32, one_hot(pick_m == 4 * iota((32, 8), 1) + u), precision=HIGH) for u in range(4)],
        axis=0,
    )

    def four_blocks(v):
        v = jnp.where(own128, v, 0.0)
        return v[0:32] + v[32:64] + v[64:96] + v[96:128]

    arrived("col", ALPHA_COL, b_in)
    shares = jnp.sum(b_in[...], axis=0) * (1.0 / NT)
    projected = four_blocks(dot(x_by_u, shares, precision=HIGH))

    arrived("row", POT_ROW, y_in)
    direct = jnp.where(own64, dot(lk[...], y_in[...].reshape(512, 128)), 0.0)
    both = fold(projected + (direct[:32] + direct[32:]) * (1.0 / NK), 64, 32)
    rows = base - jnp.where(lane_is_t, both, 0.0)
    rows = rows + pltpu.roll(rows, 31, 0)
    rows = rows + pltpu.roll(rows, 30, 0)
    for i in range(8):
        at = 128 * (i % 4)
        out_ref[i // 4 : i // 4 + 1, at : at + 128] = rows[4 * i : 4 * i + 1, :]
    alpha = fold(jnp.where(lane_is_t, dot(spread, shares, precision=HIGH), 0.0), 64, 32)
    alpha_ref[...] = (alpha + alpha_exchange)[:, :32]

    for which, many in waits:
        wait_bytes(send_sems.at[which], many)


def on_device(pair_exchange, conduction, valence, coulomb, screening, energies, vectors, k_coords):
    q2, qa, qb, m_hi, m_lo = (jnp.asarray(table) for table in tables())
    operands = (
        *(pair_exchange, conduction, valence, coulomb.reshape(1, -1), energies, vectors, k_coords),
        *(q2, qa, qb, screening, m_hi, m_lo),
    )
    vmem = pl.BlockSpec(memory_space=pltpu.VMEM)
    return pl.pallas_call(
        kernel,
        out_shape=(
            jax.ShapeDtypeStruct((2, 512), F32),
            jax.ShapeDtypeStruct((32, 32), F32),
        ),
        in_specs=[pl.BlockSpec(memory_space=pltpu.HBM)] * len(operands),
        out_specs=(vmem, vmem),
        scratch_shapes=[
            pltpu.VMEM((2, 16, 1024), BF16),
            pltpu.VMEM((2, 4, 1024), BF16),
            pltpu.VMEM((2, 4, 1024), BF16),
            pltpu.VMEM((1, 1024), F32),
            pltpu.VMEM((2, 16), F32),
            pltpu.VMEM((2, 512), BF16),
            pltpu.SMEM((2, 2), jnp.int32),
            pltpu.VMEM((32, 64), BF16),
            pltpu.VMEM((64, NK), BF16),
            pltpu.VMEM((64, NK), BF16),
            pltpu.VMEM((8, 128), F32),
            pltpu.VMEM((32, 1024), F32),
            pltpu.VMEM((64, 512), BF16),
            pltpu.VMEM((128, 256), BF16),
            pltpu.VMEM((256, 128), F32),
            pltpu.VMEM((8, 256), F32),
            pltpu.VMEM((NR, NC, 128), BF16),
            pltpu.VMEM((NR, NC, 128), BF16),
            pltpu.VMEM((NC, NR, 128), BF16),
            pltpu.VMEM((NC, NR, 128), BF16),
            pltpu.VMEM((NC, NR, 128), BF16),
            pltpu.VMEM((NC, NR, 128), BF16),
            pltpu.VMEM((NR, NC, 128), BF16),
            pltpu.VMEM((NR, NC, 128), BF16),
            pltpu.VMEM((1, 128), F32),
            pltpu.VMEM((NR, 1, 128), F32),
            pltpu.VMEM((1, 128), F32),
            pltpu.VMEM((NC, 1, 128), F32),
            pltpu.VMEM((16, 128), F32),
            pltpu.VMEM((NR, 8, 128), F32),
            pltpu.VMEM((NU, 8, 128), F32),
            pltpu.VMEM((NU, 8, 128), F32),
            pltpu.VMEM((NU, 8, 128), F32),
            pltpu.VMEM((8, 128), F32),
            pltpu.VMEM((NC, 8, 128), F32),
            pltpu.VMEM((8, 128), F32),
            pltpu.VMEM((NR, 8, 128), F32),
            pltpu.VMEM((8, 128), BF16),
            pltpu.VMEM((NR, 8, 128), BF16),
            pltpu.VMEM((8, 128), F32),
            pltpu.VMEM((NC, 8, 128), F32),
            pltpu.VMEM((2, 32, 512), F32),
            pltpu.VMEM((2, 32, 512), F32),
            pltpu.VMEM((2048, NK), BF16),
            pltpu.VMEM((2, NK, 512), BF16),
            pltpu.VMEM((2, NK, 512), BF16),
            pltpu.VMEM((8, NK), F32),
            pltpu.VMEM((64, NK), BF16),
            pltpu.VMEM((128, NK), BF16),
            pltpu.VMEM((128, 512), F32),
            pltpu.VMEM((512, 512), BF16),
            pltpu.VMEM((512, 512), BF16),
            pltpu.VMEM((2, QPAD, 128), F32),
            pltpu.VMEM((QPAD, NK), BF16),
            pltpu.VMEM((QPAD, NK), BF16),
            pltpu.SemaphoreType.DMA((13,)),
            pltpu.SemaphoreType.DMA((13,)),
            pltpu.SemaphoreType.DMA((14,)),
        ],
        compiler_params=pltpu.CompilerParams(
            collective_id=0, has_side_effects=True, vmem_limit_bytes=32 * 1024 * 1024
        ),
    )(*(pltpu.with_memory_space_constraint(v, pltpu.HBM) for v in operands))


def solution(mesh):
    split_k = ("row", "col")
    return jax.shard_map(
        on_device,
        mesh=mesh,
        in_specs=(
            P(split_k, None, None),
            P(split_k, None, None),
            P(split_k, None, None),
            P(),
            P(),
            P(split_k, None),
            P(split_k, None),
            P(split_k, None),
        ),
        out_specs=(P(split_k, None), P()),
        check_vma=False,
    )
```
